16 devices in a mesh: dp: 4 (over z, y), fsdp: 4 (over x, core).
Axes of the slice: x: 2, y: 2, z: 2, core: 2. Of those that a mesh axis runs over, the one named last changes fastest.
Arguments:
- u_in: bfloat16 [16, 512, 1536], P(('dp', 'fsdp'))
- grad_out: bfloat16 [16, 512, 1536], P(('dp', 'fsdp'))
- norm_w: bfloat16 [2, 1536], P(None, 'fsdp')
- w_in: bfloat16 [2, 1536, 6448], P(None, 'fsdp')
- conv_w: bfloat16 [2, 4, 3328], P(None, None, 'fsdp')
- conv_b: bfloat16 [2, 3328], P(None, 'fsdp')
- dt_bias: float32 [2, 48], P(None, 'fsdp')
- a_log: float32 [2, 48], P(None, 'fsdp')
- d_skip: float32 [2, 48], P(None, 'fsdp')
- gate_w: bfloat16 [2, 3072], P(None, 'fsdp')
- w_out: bfloat16 [2, 3072, 1536], P(None, 'fsdp')
Outputs:
- output 1: bfloat16 [16, 512, 1536], P(('dp', 'fsdp'))
- output 2: bfloat16 [16, 512, 1536], P(('dp', 'fsdp'))
- output 3: float32 [2, 1536], P(None, 'fsdp')
- output 4: float32 [2, 1536, 6448], P(None, 'fsdp')
- output 5: float32 [2, 4, 3328], P(None, None, 'fsdp')
- output 6: float32 [2, 3328], P(None, 'fsdp')
- output 7: float32 [2, 48], P(None, 'fsdp')
- output 8: float32 [2, 48], P(None, 'fsdp')
- output 9: float32 [2, 48], P(None, 'fsdp')
- output 10: float32 [2, 3072], P(None, 'fsdp')
- output 11: float32 [2, 3072, 1536], P(None, 'fsdp')
All inputs are finite; a program needn't handle non-finite values.
Results may differ from the reference program's by a relative error of at most 0.02.
Values are sent between devices in bfloat16 or wider.
A program may use at most 1 GiB of HBM per device.

```python
import jax
import jax.numpy as jnp
from jax import lax

D_MODEL = 1536
D_INNER = 3072
N_HEADS = 48
HEAD_DIM = 64
D_STATE = 128
N_GROUPS = 1
CONV_WIDTH = 4
CHUNK_LEN = 256
SEQ_LEN = 512
BATCH_TOT = 16
CONV_DIM = D_INNER + 2 * N_GROUPS * D_STATE
PROJ_DIM = 2 * D_INNER + 2 * N_GROUPS * D_STATE + N_HEADS
PER_GROUP = N_HEADS // N_GROUPS
NORM_EPS = 1e-5


def setup_inputs(seed: int = 0) -> dict:
    keys = jax.random.split(jax.random.key(seed), 11)

    def normal(key_i, shape, scale):
        return jax.random.normal(key_i, shape, jnp.float32) * scale

    act_shape = (BATCH_TOT, SEQ_LEN, D_MODEL)
    return {
        'u_in': normal(keys[0], act_shape, 1.0).astype(jnp.bfloat16),
        'grad_out': normal(keys[1], act_shape, 1.0).astype(jnp.bfloat16),
        'norm_w': (1.0 + normal(keys[2], (2, D_MODEL), 0.3)).astype(jnp.bfloat16),
        'w_in': normal(keys[3], (2, D_MODEL, PROJ_DIM), D_MODEL ** -0.5).astype(jnp.bfloat16),
        'conv_w': normal(keys[4], (2, CONV_WIDTH, CONV_DIM), CONV_WIDTH ** -0.5).astype(jnp.bfloat16),
        'conv_b': normal(keys[5], (2, CONV_DIM), 0.5).astype(jnp.bfloat16),
        'dt_bias': normal(keys[6], (2, N_HEADS), 1.0) - 2.0,
        'a_log': jnp.log(jax.random.uniform(keys[7], (2, N_HEADS), jnp.float32, 1.0, 16.0)),
        'd_skip': 1.0 + normal(keys[8], (2, N_HEADS), 0.5),
        'gate_w': (1.0 + normal(keys[9], (2, D_INNER), 0.3)).astype(jnp.bfloat16),
        'w_out': normal(keys[10], (2, D_INNER, D_MODEL), D_INNER ** -0.5).astype(jnp.bfloat16),
    }


def pre_norm(u_rows, norm_w):
    rows_f = u_rows.astype(jnp.float32)
    inv_rms = lax.rsqrt(jnp.mean(rows_f * rows_f, axis=-1, keepdims=True) + NORM_EPS)
    return (rows_f * inv_rms * norm_w.astype(jnp.float32)).astype(jnp.bfloat16)


def ssd_chunks(x_heads, dt_heads, a_heads, b_mat, c_mat):
    n_chunks = x_heads.shape[0] // CHUNK_LEN
    x_dt = (x_heads * dt_heads[:, :, None]).reshape(n_chunks, CHUNK_LEN, N_GROUPS, PER_GROUP, HEAD_DIM)
    cum_a = jnp.cumsum(a_heads.reshape(n_chunks, CHUNK_LEN, N_GROUPS, PER_GROUP), axis=1)
    b_chunk = b_mat.reshape(n_chunks, CHUNK_LEN, N_GROUPS, D_STATE).astype(jnp.float32)
    c_chunk = c_mat.reshape(n_chunks, CHUNK_LEN, N_GROUPS, D_STATE).astype(jnp.float32)
    scores = jnp.einsum('cqgn,csgn->cgqs', c_chunk, b_chunk)
    cum_t = jnp.moveaxis(cum_a, 1, -1)
    log_gap = cum_t[..., :, None] - cum_t[..., None, :]
    causal = jnp.arange(CHUNK_LEN)[:, None] >= jnp.arange(CHUNK_LEN)[None, :]
    decay_mat = jnp.where(causal, jnp.exp(jnp.where(causal, log_gap, 0.0)), 0.0)
    y_diag = jnp.einsum('cgrqs,csgrp->cqgrp', scores[:, :, None] * decay_mat, x_dt)
    end_decay = jnp.exp(cum_a[:, -1:] - cum_a)
    states = jnp.einsum('csgn,csgrp->cgrpn', b_chunk, x_dt * end_decay[..., None])
    totals = cum_a[:, -1]
    incl_sum = jnp.cumsum(totals, axis=0)
    excl_sum = incl_sum - totals
    chunk_gap = jnp.moveaxis(excl_sum, 0, -1)[..., :, None] - jnp.moveaxis(incl_sum, 0, -1)[..., None, :]
    earlier = jnp.arange(n_chunks)[:, None] > jnp.arange(n_chunks)[None, :]
    carry_mat = jnp.where(earlier, jnp.exp(jnp.where(earlier, chunk_gap, 0.0)), 0.0)
    prev_state = jnp.einsum('grij,jgrpn->igrpn', carry_mat, states)
    y_off = jnp.einsum('cqgn,cgrpn->cqgrp', c_chunk, prev_state) * jnp.exp(cum_a)[..., None]
    return (y_diag + y_off).reshape(x_heads.shape)


def mamba_layer(u_seq, layer_w):
    norm_w, w_in, conv_w, conv_b, dt_bias, a_log, d_skip, gate_w, w_out = layer_w
    seq_len = u_seq.shape[0]
    h_norm = pre_norm(u_seq, norm_w)
    proj_out = jnp.dot(h_norm, w_in, preferred_element_type=jnp.float32).astype(jnp.bfloat16)
    xbc = proj_out[:, D_INNER:D_INNER + CONV_DIM].astype(jnp.float32)
    padded = jnp.pad(xbc, ((CONV_WIDTH - 1, 0), (0, 0)))
    conv_out = conv_b.astype(jnp.float32) + sum(padded[tap:tap + seq_len] * conv_w[tap].astype(jnp.float32) for tap in range(CONV_WIDTH))
    xbc_act = jax.nn.silu(conv_out)
    group_w = N_GROUPS * D_STATE
    x_heads = xbc_act[:, :D_INNER].reshape(seq_len, N_HEADS, HEAD_DIM)
    b_mat = xbc_act[:, D_INNER:D_INNER + group_w].reshape(seq_len, N_GROUPS, D_STATE)
    c_mat = xbc_act[:, D_INNER + group_w:].reshape(seq_len, N_GROUPS, D_STATE)
    dt_heads = jax.nn.softplus(proj_out[:, D_INNER + CONV_DIM:].astype(jnp.float32) + dt_bias)
    a_heads = dt_heads * -jnp.exp(a_log)
    y_heads = ssd_chunks(x_heads, dt_heads, a_heads, b_mat, c_mat) + d_skip[:, None] * x_heads
    z_act = jax.nn.silu(proj_out[:, :D_INNER].astype(jnp.float32))
    gated_y = y_heads.reshape(seq_len, N_GROUPS, -1) * z_act.reshape(seq_len, N_GROUPS, -1)
    normed = gated_y * lax.rsqrt(jnp.mean(gated_y * gated_y, axis=-1, keepdims=True) + NORM_EPS)
    y_norm = (normed.reshape(seq_len, D_INNER) * gate_w.astype(jnp.float32)).astype(jnp.bfloat16)
    mixed = jnp.dot(y_norm, w_out, preferred_element_type=jnp.float32)
    return (u_seq.astype(jnp.float32) + mixed).astype(jnp.bfloat16)


def reference(u_in, grad_out, norm_w, w_in, conv_w, conv_b, dt_bias, a_log, d_skip, gate_w, w_out):
    params = (norm_w, w_in, conv_w, conv_b, dt_bias, a_log, d_skip, gate_w, w_out)

    def two_layers(u_seq, stack_w):
        hidden = mamba_layer(u_seq, [w_l[0] for w_l in stack_w])
        return mamba_layer(hidden, [w_l[1] for w_l in stack_w])

    def per_sequence(acc, pair):
        u_seq, g_seq = pair
        out_seq, pull = jax.vjp(two_layers, u_seq, params)
        du_seq, d_params = pull(g_seq)
        acc = tuple(total + grad_w.astype(jnp.float32) for total, grad_w in zip(acc, d_params))
        return acc, (out_seq, du_seq)

    zeros = tuple(jnp.zeros(w_l.shape, jnp.float32) for w_l in params)
    sums, (out, d_u) = lax.scan(per_sequence, zeros, (u_in, grad_out))
    return (out, d_u) + tuple(total / BATCH_TOT for total in sums)
```

```python
import jax
import jax.numpy as jnp
from jax import lax
from jax.experimental import pallas as pl
from jax.experimental.pallas import tpu as pltpu
from jax.sharding import PartitionSpec as P


CHUNK = 256
SEQ = 512
LANES = 128
HEAD = 64
D_MODEL = 1536
D_INNER = 3072
N_HEADS = 48
CONV_DIM = 3328
PROJ = 6448
PROJ_PAD = 6528
N_PAIRS = N_HEADS // 2
NORM_EPS = 1e-5
F32 = jnp.float32
BF16 = jnp.bfloat16
NT = (((1,), (1,)), ((), ()))
TN = (((0,), (0,)), ((), ()))


def _dot(a, b):
    return jnp.dot(a, b, preferred_element_type=F32)


def _dot_dims(a, b, dims):
    return lax.dot_general(a, b, dims, preferred_element_type=F32)


def _iota(shape, dim):
    return lax.broadcasted_iota(jnp.int32, shape, dim)


def _later(x, k):
    if k == 0:
        return x
    return jnp.where(_iota(x.shape, 0) >= k, pltpu.roll(x, k, 0), 0.0)


def _sooner(x, k):
    if k == 0:
        return x
    n = x.shape[0]
    return jnp.where(_iota(x.shape, 0) < n - k, pltpu.roll(x, n - k, 0), 0.0)


def _conv(x_in, taps):
    out = taps[4:5] + x_in * taps[3:4]
    for k in range(3):
        out += _later(x_in, 3 - k) * taps[k:k + 1]
    return out


def _conv_back(d_out, x_in, taps):
    d_in = d_out * taps[3:4]
    for k in range(3):
        d_in += _sooner(d_out, 3 - k) * taps[k:k + 1]
    rows = [jnp.sum(d_out * _later(x_in, 3 - k), axis=0, keepdims=True) for k in range(4)]
    rows.append(jnp.sum(d_out, axis=0, keepdims=True))
    return d_in, rows


def _sigmoid(x):
    return 1.0 / (1.0 + jnp.exp(-x))


def _silu_grad(x, sig):
    return sig * (1.0 + x * (1.0 - sig))


def _pair(a, b):
    shape = (max(a.shape[0], b.shape[0]), LANES)
    return jnp.where(_iota(shape, 1) < HEAD, a, b)


def _scores(b_ref, c_ref, tb_ref, tc_ref, b_sc, c_sc, g_sc):
    for ref, taps, dst in ((b_ref, tb_ref, b_sc), (c_ref, tc_ref, c_sc)):
        pre = _conv(ref[...].astype(F32), taps[...])
        dst[...] = (pre * _sigmoid(pre)).astype(BF16)
    causal = _iota((CHUNK, CHUNK), 0) >= _iota((CHUNK, CHUNK), 1)
    for c in range(2):
        sl = pl.ds(c * CHUNK, CHUNK)
        g_sc[c] = jnp.where(causal, _dot_dims(c_sc[sl, :], b_sc[sl, :], NT), 0.0)


def _decay(rows, cols, c, h):
    lo, hi = c * CHUNK, (c + 1) * CHUNK
    return jnp.exp(jnp.minimum(cols[lo:hi, 2 + h:3 + h] - rows[2 + h:3 + h, lo:hi], 0.0))


def _state(x_dt, rows, cols, b_sc):
    end = _pair(rows[2:3, CHUNK - 1:CHUNK], rows[3:4, CHUNK - 1:CHUNK])
    weight = jnp.exp(jnp.minimum(end - _pair(cols[:CHUNK, 2:3], cols[:CHUNK, 3:4]), 0.0))
    x_end = (x_dt[:CHUNK] * weight).astype(BF16)
    state = _dot_dims(x_end, b_sc[pl.ds(0, CHUNK), :], TN).astype(BF16)
    return state, x_end, weight


def fwd_kernel(rows_ref, x_ref, z_ref, b_ref, c_ref, tx_ref, tb_ref, tc_ref, par_ref,
               y_ref, n_ref, r_ref, b_sc, c_sc, g_sc, v_sc, acc):
    j = pl.program_id(0)

    @pl.when(j == 0)
    def _():
        _scores(b_ref, c_ref, tb_ref, tc_ref, b_sc, c_sc, g_sc)
        acc[...] = jnp.zeros_like(acc)

    rows = rows_ref[0]
    cols = rows.T
    pre = _conv(x_ref[...].astype(F32), tx_ref[...])
    x = pre * _sigmoid(pre)
    x_dt = x * _pair(cols[:, 0:1], cols[:, 1:2])
    x_b = x_dt.astype(BF16)
    y_parts = []
    for c in range(2):
        lo, hi = c * CHUNK, (c + 1) * CHUNK
        heads = [_dot((g_sc[c] * _decay(rows, cols, c, h)).astype(BF16), x_b[lo:hi]) for h in range(2)]
        y_parts.append(_pair(heads[0], heads[1]))
    state, _, _ = _state(x_dt, rows, cols, b_sc)
    from_start = jnp.exp(_pair(cols[CHUNK:, 2:3], cols[CHUNK:, 3:4]))
    y_parts[1] += from_start * _dot_dims(c_sc[pl.ds(CHUNK, CHUNK), :], state, NT)
    lane0 = pl.multiple_of(j * LANES, LANES)
    y = jnp.concatenate(y_parts, axis=0) + par_ref[1:2, pl.ds(lane0, LANES)] * x
    y_ref[...] = y
    z = z_ref[...].astype(F32)
    v = y * (z * _sigmoid(z))
    v_sc[j] = v
    acc[...] += v * v

    @pl.when(j == N_PAIRS - 1)
    def _():
        r = lax.rsqrt(jnp.sum(acc[...], axis=1, keepdims=True) / D_INNER + NORM_EPS)
        r_full = jnp.broadcast_to(r, (SEQ, LANES))
        r_ref[...] = r_full

        @pl.loop(0, N_PAIRS)
        def _(i):
            at = pl.ds(pl.multiple_of(i * LANES, LANES), LANES)
            n_ref[:, at] = (v_sc[i] * r_full * par_ref[0:1, at]).astype(BF16)


def bwd_kernel(rows_ref, x_ref, z_ref, b_ref, c_ref, y_ref, dn_ref, r_ref, tx_ref, tb_ref, tc_ref, par_ref,
               dp_ref, drows_ref, gch_ref, gbc_ref, b_sc, c_sc, g_sc, dg_sc, dc_sc, db_sc, acc):
    phase, j = pl.program_id(0), pl.program_id(1)
    gate = par_ref[0:1]
    skip = par_ref[1:2]
    z = z_ref[...].astype(F32)
    sig_z = _sigmoid(z)
    act_z = z * sig_z
    y = y_ref[...]
    v = y * act_z
    d_n = dn_ref[...].astype(F32)
    d_vn = d_n * gate

    @pl.when(phase == 0)
    def _():
        @pl.when(j == 0)
        def _():
            acc[...] = jnp.zeros_like(acc)

        acc[...] += d_vn * v

    @pl.when(phase == 1)
    def _():
        @pl.when(j == 0)
        def _():
            total = jnp.sum(acc[...], axis=1, keepdims=True) / D_INNER
            acc[...] = jnp.broadcast_to(total, (SEQ, LANES))
            _scores(b_ref, c_ref, tb_ref, tc_ref, b_sc, c_sc, g_sc)
            dg_sc[...] = jnp.zeros_like(dg_sc)
            dc_sc[...] = jnp.zeros_like(dc_sc)
            db_sc[...] = jnp.zeros_like(db_sc)

        r = r_ref[...]
        d_v = r * d_vn - v * (r * r * r) * acc[...]
        g_gate = jnp.sum(d_n * v * r, axis=0, keepdims=True)
        lane0 = pl.multiple_of(j * LANES, LANES)
        dp_ref[:, pl.ds(lane0, LANES)] = (d_v * y * _silu_grad(z, sig_z)).astype(BF16)
        d_y = d_v * act_z

        rows = rows_ref[0]
        cols = rows.T
        x_in = x_ref[...].astype(F32)
        pre = _conv(x_in, tx_ref[...])
        sig_x = _sigmoid(pre)
        x = pre * sig_x
        dt = _pair(cols[:, 0:1], cols[:, 1:2])
        x_dt = x * dt
        x_b = x_dt.astype(BF16)
        x_r = x_b.astype(F32)
        g_skip = jnp.sum(d_y * x, axis=0, keepdims=True)
        dy_b = d_y.astype(BF16)
        dy_r = dy_b.astype(F32)
        dy_t = dy_r.T.astype(BF16)
        first = _iota((CHUNK, LANES), 1) < HEAD
        dx_parts = []
        for c in range(2):
            lo, hi = c * CHUNK, (c + 1) * CHUNK
            halves = []
            for h in range(2):
                decay = _decay(rows, cols, c, h)
                mixed = (g_sc[c] * decay).astype(BF16)
                own = first if h == 0 else jnp.logical_not(first)
                dy_h = jnp.where(own, dy_r[lo:hi], 0.0).astype(BF16)
                dg_sc[c] += _dot_dims(dy_h, x_b[lo:hi], NT) * decay
                halves.append(_dot(dy_t[h * HEAD:(h + 1) * HEAD, lo:hi], mixed))
            dx_parts.append(jnp.concatenate(halves, axis=0).T)
        state, x_end, weight = _state(x_dt, rows, cols, b_sc)
        dy_off = dy_r[CHUNK:] * jnp.exp(_pair(cols[CHUNK:, 2:3], cols[CHUNK:, 3:4]))
        dc_sc[...] += _dot(dy_off.astype(BF16), state)
        d_state = _dot(dy_off.T.astype(BF16), c_sc[pl.ds(CHUNK, CHUNK), :]).astype(BF16)
        db_sc[...] += _dot(x_end, d_state)
        dx_state = weight * _dot_dims(b_sc[pl.ds(0, CHUNK), :], d_state, NT)
        dx_parts[0] += dx_state
        d_xdt = jnp.concatenate(dx_parts, axis=0)
        end_sum = jnp.sum(x_r[:CHUNK] * dx_state, axis=0, keepdims=True)
        d_cum = dy_r * (y - skip * x) - x_r * d_xdt
        d_cum += jnp.where(_iota((SEQ, LANES), 0) == CHUNK - 1, end_sum, 0.0)
        dt_t = (d_xdt * x).T
        cum_t = d_cum.T
        drows_ref[0] = jnp.concatenate(
            [jnp.sum(part[h * HEAD:(h + 1) * HEAD], axis=0, keepdims=True) for part in (dt_t, cum_t) for h in range(2)]
            + [jnp.zeros((4, SEQ), F32)], axis=0)
        d_pre = (d_xdt * dt + skip * d_y) * _silu_grad(pre, sig_x)
        d_in, g_rows = _conv_back(d_pre, x_in, tx_ref[...])
        dp_ref[:, pl.ds(pl.multiple_of(D_INNER + lane0, LANES), LANES)] = d_in.astype(BF16)
        gch_ref[...] = jnp.concatenate(g_rows + [g_gate, g_skip, jnp.zeros((1, LANES), F32)], axis=0)

        @pl.when(j == N_PAIRS - 1)
        def _():
            causal = _iota((CHUNK, CHUNK), 0) >= _iota((CHUNK, CHUNK), 1)
            d_b, d_c = [], []
            for c in range(2):
                sl = pl.ds(c * CHUNK, CHUNK)
                d_g = jnp.where(causal, dg_sc[c], 0.0)
                d_c.append(_dot(d_g.astype(BF16), b_sc[sl, :]))
                d_b.append(_dot(d_g.T.astype(BF16), c_sc[sl, :]))
            d_c[1] += dc_sc[...]
            d_b[0] += db_sc[...]
            for i, (parts, ref, taps) in enumerate(((d_b, b_ref, tb_ref), (d_c, c_ref, tc_ref))):
                val = ref[...].astype(F32)
                pre_i = _conv(val, taps[...])
                d_pre_i = jnp.concatenate(parts, axis=0) * _silu_grad(pre_i, _sigmoid(pre_i))
                d_val, g_val = _conv_back(d_pre_i, val, taps[...])
                dp_ref[:, pl.ds(2 * D_INNER + i * LANES, LANES)] = d_val.astype(BF16)
                gbc_ref[:, pl.ds(i * LANES, LANES)] = jnp.concatenate(g_val + [jnp.zeros((3, LANES), F32)], axis=0)
            dp_ref[:, pl.ds(2 * D_INNER + 2 * LANES, LANES)] = jnp.zeros((SEQ, LANES), BF16)


def _col(block):
    return pl.BlockSpec((SEQ, LANES), lambda j: (0, block(j)))


def part_rows(rows):
    return -(-rows // 64) * 16


def mixer_fwd(proj, rows, taps, par):
    taps_at = lambda block: pl.BlockSpec((8, LANES), lambda j: (0, block(j)))
    return pl.pallas_call(
        fwd_kernel,
        grid=(N_PAIRS,),
        in_specs=[
            pl.BlockSpec((1, 8, SEQ), lambda j: (j, 0, 0)),
            _col(lambda j: N_PAIRS + j), _col(lambda j: j), _col(lambda j: 2 * N_PAIRS), _col(lambda j: 2 * N_PAIRS + 1),
            taps_at(lambda j: j), taps_at(lambda j: N_PAIRS), taps_at(lambda j: N_PAIRS + 1),
            pl.BlockSpec((8, D_INNER), lambda j: (0, 0)),
        ],
        out_specs=[_col(lambda j: j), pl.BlockSpec((SEQ, D_INNER), lambda j: (0, 0)), pl.BlockSpec((SEQ, LANES), lambda j: (0, 0))],
        out_shape=[
            jax.ShapeDtypeStruct((SEQ, D_INNER), F32),
            jax.ShapeDtypeStruct((SEQ, D_INNER), BF16),
            jax.ShapeDtypeStruct((SEQ, LANES), F32),
        ],
        scratch_shapes=[
            pltpu.VMEM((SEQ, LANES), BF16), pltpu.VMEM((SEQ, LANES), BF16), pltpu.VMEM((2, CHUNK, CHUNK), F32),
            pltpu.VMEM((N_PAIRS, SEQ, LANES), F32), pltpu.VMEM((SEQ, LANES), F32),
        ],
        compiler_params=pltpu.CompilerParams(dimension_semantics=("arbitrary",), vmem_limit_bytes=40 * 2 ** 20),
        cost_estimate=pl.CostEstimate(flops=8 * 10 ** 9, bytes_accessed=16 * 10 ** 6, transcendentals=10 ** 7),
        name="mixer_fwd",
    )(rows, proj, proj, proj, proj, taps, taps, taps, par)


def mixer_bwd(proj, rows, taps, par, y, d_n, r):
    col = lambda block: pl.BlockSpec((SEQ, LANES), lambda f, j: (0, block(f, j)))
    taps_at = lambda block: pl.BlockSpec((8, LANES), lambda f, j: (0, block(f, j)))
    return pl.pallas_call(
        bwd_kernel,
        grid=(2, N_PAIRS),
        in_specs=[
            pl.BlockSpec((1, 8, SEQ), lambda f, j: (f * j, 0, 0)),
            col(lambda f, j: N_PAIRS + f * j), col(lambda f, j: j), col(lambda f, j: 2 * N_PAIRS), col(lambda f, j: 2 * N_PAIRS + 1),
            col(lambda f, j: j), col(lambda f, j: j), col(lambda f, j: 0),
            taps_at(lambda f, j: f * j), taps_at(lambda f, j: N_PAIRS), taps_at(lambda f, j: N_PAIRS + 1), taps_at(lambda f, j: j),
        ],
        out_specs=[
            pl.BlockSpec((SEQ, PROJ_PAD), lambda f, j: (0, 0)),
            pl.BlockSpec((1, 8, SEQ), lambda f, j: (f * j, 0, 0)),
            taps_at(lambda f, j: f * j),
            pl.BlockSpec((8, 2 * LANES), lambda f, j: (0, 0)),
        ],
        out_shape=[
            jax.ShapeDtypeStruct((SEQ, PROJ_PAD), BF16),
            jax.ShapeDtypeStruct((N_PAIRS, 8, SEQ), F32),
            jax.ShapeDtypeStruct((8, D_INNER), F32),
            jax.ShapeDtypeStruct((8, 2 * LANES), F32),
        ],
        scratch_shapes=[
            pltpu.VMEM((SEQ, LANES), BF16), pltpu.VMEM((SEQ, LANES), BF16), pltpu.VMEM((2, CHUNK, CHUNK), F32),
            pltpu.VMEM((2, CHUNK, CHUNK), F32), pltpu.VMEM((CHUNK, LANES), F32), pltpu.VMEM((CHUNK, LANES), F32),
            pltpu.VMEM((SEQ, LANES), F32),
        ],
        compiler_params=pltpu.CompilerParams(dimension_semantics=("arbitrary", "arbitrary"), vmem_limit_bytes=40 * 2 ** 20),
        cost_estimate=pl.CostEstimate(flops=16 * 10 ** 9, bytes_accessed=40 * 10 ** 6, transcendentals=10 ** 7),
        name="mixer_bwd",
    )(rows, proj, proj, proj, proj, y, d_n, r, taps, taps, taps, par)


def pre_norm(u_rows, norm_w):
    rows_f = u_rows.astype(F32)
    inv_rms = lax.rsqrt(jnp.mean(jnp.square(rows_f), axis=-1, keepdims=True) + NORM_EPS)
    return (rows_f * inv_rms * norm_w.astype(F32)).astype(BF16)


def head_rows(dt_raw, dt_bias, a_log):
    dt = jax.nn.softplus(dt_raw.astype(F32) + dt_bias).T
    a = dt * -jnp.exp(a_log)[:, None]
    upto = (jnp.arange(CHUNK)[:, None] <= jnp.arange(CHUNK)[None, :]).astype(F32)
    cum = jnp.einsum('hcs,st->hct', a.reshape(N_HEADS, SEQ // CHUNK, CHUNK), upto, precision=lax.Precision.HIGHEST)
    pairs = (N_PAIRS, 2, SEQ)
    return jnp.concatenate([dt.reshape(pairs), cum.reshape(pairs), jnp.zeros((N_PAIRS, 4, SEQ), F32)], axis=1)


def layer_forward(u_rows, small, w_in, w_out):
    norm_w, taps, par, dt_bias, a_log = small
    h_norm, norm_pull = jax.vjp(pre_norm, u_rows, norm_w)
    proj = jnp.dot(h_norm, w_in, preferred_element_type=F32).astype(BF16)
    rows, rows_pull = jax.vjp(head_rows, proj[:, 2 * D_INNER + 2 * LANES:], dt_bias, a_log)
    y, y_norm, r = mixer_fwd(proj, rows, taps, par)
    out = (u_rows.astype(F32) + jnp.dot(y_norm, w_out, preferred_element_type=F32)).astype(BF16)
    return out, (h_norm, norm_pull, proj, rows, rows_pull, y, y_norm, r)


COL_CHUNKS = ((0, 2176), (2176, 4352), (4352, 6528))


def solution(mesh):
    dp_size = mesh.shape['dp']
    fsdp_size = mesh.shape['fsdp']
    act_spec = P(('dp', 'fsdp'), None, None)
    weight_specs = (P(None, 'fsdp'), P(None, 'fsdp', None), P(None, None, 'fsdp'), P(None, 'fsdp'), P(None, 'fsdp'), P(None, 'fsdp'), P(None, 'fsdp'), P(None, 'fsdp'), P(None, 'fsdp', None))

    def per_device(u_loc, g_loc, norm_w, w_in, conv_w, conv_b, dt_bias, a_log, d_skip, gate_w, w_out):
        batch_tot = dp_size * fsdp_size
        me_dp = lax.axis_index('dp')
        me_fsdp = lax.axis_index('fsdp')

        small_pieces = [norm_w, conv_w.reshape(2, -1), conv_b, gate_w, dt_bias, a_log, d_skip]
        widths = [piece.shape[1] for piece in small_pieces]
        packed = jnp.concatenate([piece.astype(F32) for piece in small_pieces], axis=1)
        gathered = lax.all_gather(packed, 'fsdp', axis=0)

        def small_layer(layer):
            vals, at = [], 0
            for width in widths:
                vals.append(gathered[:, layer, at:at + width])
                at += width
            norm, cw, cb, gate, bias, alog, skip = vals
            taps = jnp.concatenate([
                cw.reshape(fsdp_size, 4, -1).transpose(1, 0, 2).reshape(4, CONV_DIM), cb.reshape(1, CONV_DIM),
                jnp.zeros((3, CONV_DIM), F32)], axis=0)
            par = jnp.concatenate([
                gate.reshape(1, D_INNER), jnp.repeat(skip.reshape(N_HEADS), HEAD).reshape(1, D_INNER),
                jnp.zeros((6, D_INNER), F32)], axis=0)
            return norm.reshape(D_MODEL), taps, par, bias.reshape(N_HEADS), alog.reshape(N_HEADS)

        def gather_in_order(pieces):
            full, fulls = None, []
            for piece in pieces:
                if full is not None:
                    piece, full = lax.optimization_barrier((piece, full))
                    fulls.append(full)
                full = lax.all_gather(piece, 'fsdp', axis=0, tiled=True)
            return fulls + [full]

        def partial_grad(left, right):
            return (lax.dot_general(left, right, TN, preferred_element_type=F32) / batch_tot).astype(BF16)

        def spread(part, flip=False, valid=None):
            piece = lax.psum_scatter(part, 'fsdp', scatter_dimension=0, tiled=True)
            piece = piece.T if flip else piece
            rows = piece.shape[0] if valid is None else valid
            size = part_rows(rows)

            def quarter(k):
                return lax.dynamic_slice_in_dim(piece, jnp.minimum((me_dp ^ k) * size, rows - size), size, 0)

            sent = [quarter(k) for k in range(dp_size)]
            terms = sent[:1]
            for k in range(1, dp_size):
                terms.append(lax.ppermute(sent[k], 'dp', [(i, i ^ k) for i in range(dp_size)]))
            terms = [term.astype(F32) for term in terms]
            total = (terms[0] + terms[1]) + (terms[2] + terms[3])
            return [total] + [lax.ppermute(total, 'dp', [(i, i ^ k) for i in range(dp_size)]) for k in range(1, dp_size)]

        def place(buf, layer, parts, first, rows):
            for k, part in enumerate(parts):
                row = first + jnp.minimum((me_dp ^ k) * part.shape[0], rows - part.shape[0])
                buf = lax.dynamic_update_slice(buf, part[None], (layer, row, 0))
            return buf

        def layer_backward(d_out, saved, small, full_in, full_out):
            _, taps, par, _, _ = small
            h_norm, norm_pull, proj, rows, rows_pull, y, y_norm, r = saved
            g_out_part = partial_grad(y_norm, d_out)
            d_out, g_out_part = lax.optimization_barrier((d_out, g_out_part))
            out_parts = spread(g_out_part)
            d_n = lax.dot_general(d_out, full_out, NT, preferred_element_type=F32).astype(BF16)
            d_proj, d_rows, g_ch, g_bc = mixer_bwd(proj, rows, taps, par, y, d_n, r)
            d_raw, g_bias, g_alog = rows_pull(d_rows)
            d_proj = lax.dynamic_update_slice(d_proj, d_raw, (0, 2 * D_INNER + 2 * LANES))
            g_in_parts = [partial_grad(h_norm, d_proj[:, lo:hi]) for lo, hi in COL_CHUNKS]
            d_proj, g_in_parts = lax.optimization_barrier((d_proj, g_in_parts))
            in_parts = [spread(part, flip=True, valid=min(hi, PROJ) - lo) for part, (lo, hi) in zip(g_in_parts, COL_CHUNKS)]
            d_h = lax.dot_general(d_proj[:, :PROJ], full_in, NT, preferred_element_type=F32).astype(BF16)
            d_u_norm, g_norm = norm_pull(d_h)
            d_u = (d_out.astype(F32) + d_u_norm.astype(F32)).astype(BF16)
            g_conv = jnp.concatenate([g_ch[:5], g_bc[:5]], axis=1)
            g_skip = jnp.sum(g_ch[6].reshape(N_HEADS, HEAD), axis=1)
            smalls = [g_norm, g_conv[:4], g_conv[4], g_ch[5], g_bias, g_alog, g_skip]
            return d_u, out_parts, in_parts, smalls

        u_rows, d_out = u_loc[0], g_loc[0]
        small_one, small_two = small_layer(0), small_layer(1)
        in_one, out_one, in_two, out_two = gather_in_order([w_in[0], w_out[0], w_in[1], w_out[1]])
        hidden, saved_one = layer_forward(u_rows, small_one, in_one, out_one)
        out_rows, saved_two = layer_forward(hidden, small_two, in_two, out_two)
        d_hidden, out_parts_two, in_parts_two, smalls_two = layer_backward(d_out, saved_two, small_two, in_two, out_two)
        d_u, out_parts_one, in_parts_one, smalls_one = layer_backward(d_hidden, saved_one, small_one, in_one, out_one)

        g_in = jnp.zeros((2, PROJ, w_in.shape[1]), F32)
        g_out = jnp.zeros((2,) + w_out.shape[1:], F32)
        g_out = place(g_out, 1, out_parts_two, 0, g_out.shape[1])
        for (lo, hi), parts in zip(COL_CHUNKS, in_parts_two):
            g_in = place(g_in, 1, parts, lo, min(hi, PROJ) - lo)
        g_out = place(g_out, 0, out_parts_one, 0, g_out.shape[1])
        for (lo, hi), parts in zip(COL_CHUNKS, in_parts_one):
            g_in = place(g_in, 0, parts, lo, min(hi, PROJ) - lo)

        def small_piece_rows(smalls):
            vals = []
            for idx, grad in enumerate(smalls):
                grad = grad.astype(F32) / batch_tot
                if idx < 4:
                    grad = grad.astype(BF16).astype(F32)
                if idx == 1:
                    grad = grad.reshape(4, fsdp_size, -1).transpose(1, 0, 2)
                vals.append(grad.reshape(fsdp_size, -1))
            return jnp.concatenate(vals, axis=1)

        both = jnp.stack([small_piece_rows(smalls_one), small_piece_rows(smalls_two)], axis=1)
        for axis in ('fsdp', 'dp'):
            for k in (1, 2):
                both = both + lax.ppermute(both, axis, [(i, i ^ k) for i in range(4)])
        summed = lax.dynamic_index_in_dim(both, me_fsdp, 0, keepdims=False)
        outs, at = [], 0
        for width in widths:
            outs.append(summed[:, at:at + width])
            at += width
        g_norm, g_cw, g_cb, g_gate, g_bias, g_alog, g_skip = outs
        return (out_rows[None], d_u[None], g_norm, g_in.swapaxes(1, 2), g_cw.reshape(conv_w.shape), g_cb, g_bias, g_alog, g_skip, g_gate, g_out)

    return jax.shard_map(per_device, mesh=mesh, in_specs=(act_spec, act_spec) + weight_specs, out_specs=(act_spec, act_spec) + weight_specs, check_vma=False)
```

```python
import jax
import jax.numpy as jnp
from jax import lax
from jax.experimental import pallas as pl
from jax.experimental.pallas import tpu as pltpu
from jax.sharding import PartitionSpec as P


ALL = Ellipsis
CHUNK = 256
SEQ = 512
LANES = 128
PAD = 8
HEAD = 64
D_MODEL = 1536
D_INNER = 3072
N_HEADS = 48
CONV_DIM = 3328
PROJ = 6448
PROJ_PAD = 6528
N_PAIRS = N_HEADS // 2
NORM_EPS = 1e-5
F32 = jnp.float32
BF16 = jnp.bfloat16
NT = (((1,), (1,)), ((), ()))
TN = (((0,), (0,)), ((), ()))


def _dot(a, b):
    return jnp.dot(a, b, preferred_element_type=F32)


def _dot_dims(a, b, dims):
    return lax.dot_general(a, b, dims, preferred_element_type=F32)


def _sum(x, axis):
    return jnp.sum(x, axis=axis, keepdims=True)


def _iota(shape, dim):
    return lax.broadcasted_iota(jnp.int32, shape, dim)


def _fill(pad, x):
    zeros = jnp.zeros((PAD, LANES), F32)
    pad[pl.ds(0, PAD), :] = zeros
    pad[pl.ds(PAD, SEQ), :] = x
    pad[pl.ds(PAD + SEQ, PAD), :] = zeros


def _shift(pad, k):
    return pad[pl.ds(PAD + k, SEQ), :]


def _conv(pad, taps):
    out = taps[4:5] + _shift(pad, 0) * taps[3:4]
    for k in range(3):
        out += _shift(pad, k - 3) * taps[k:k + 1]
    return out


def _conv_back(pad_out, d_out, pad_in, taps):
    _fill(pad_out, d_out)
    d_in = d_out * taps[3:4]
    for k in range(3):
        d_in += _shift(pad_out, 3 - k) * taps[k:k + 1]
    rows = [_sum(d_out * _shift(pad_in, k - 3), 0) for k in range(4)]
    rows.append(_sum(d_out, 0))
    return d_in, rows


def _sigmoid(x):
    return 0.5 * jnp.tanh(0.5 * x) + 0.5


def _silu_grad(x, sig):
    return sig * (1.0 + x * (1.0 - sig))


def _pair(a, b):
    shape = (max(a.shape[0], b.shape[0]), LANES)
    return jnp.where(_iota(shape, 1) < HEAD, a, b)


def _scores(b_ref, c_ref, tb_ref, tc_ref, b_sc, c_sc, g_sc, pad):
    for ref, taps, dst in ((b_ref, tb_ref, b_sc), (c_ref, tc_ref, c_sc)):
        _fill(pad, ref[ALL].astype(F32))
        pre = _conv(pad, taps[ALL])
        dst[ALL] = (pre * _sigmoid(pre)).astype(BF16)
    causal = _iota((CHUNK, CHUNK), 0) >= _iota((CHUNK, CHUNK), 1)
    for c in range(2):
        sl = pl.ds(c * CHUNK, CHUNK)
        g_sc[c] = jnp.where(causal, _dot_dims(c_sc[sl, :], b_sc[sl, :], NT), 0.0)


def _decay(rows, cols, c, h):
    lo, hi = c * CHUNK, (c + 1) * CHUNK
    return jnp.exp(jnp.minimum(cols[lo:hi, 2 + h:3 + h] - rows[2 + h:3 + h, lo:hi], 0.0))


def _state(x_dt, rows, cols, b_sc):
    end = _pair(rows[2:3, CHUNK - 1:CHUNK], rows[3:4, CHUNK - 1:CHUNK])
    weight = jnp.exp(jnp.minimum(end - _pair(cols[:CHUNK, 2:3], cols[:CHUNK, 3:4]), 0.0))
    x_end = (x_dt[:CHUNK] * weight).astype(BF16)
    state = _dot_dims(x_end, b_sc[pl.ds(0, CHUNK), :], TN).astype(BF16)
    return state, x_end, weight


def fwd_kernel(rows_ref, x_ref, z_ref, b_ref, c_ref, tx_ref, tb_ref, tc_ref, par_ref,
               y_ref, n_ref, r_ref, b_sc, c_sc, g_sc, v_sc, acc, pad):
    j = pl.program_id(0)

    @pl.when(j == 0)
    def _():
        _scores(b_ref, c_ref, tb_ref, tc_ref, b_sc, c_sc, g_sc, pad)
        acc[ALL] = jnp.zeros_like(acc)

    rows = rows_ref[0]
    cols = rows.T
    _fill(pad, x_ref[ALL].astype(F32))
    pre = _conv(pad, tx_ref[ALL])
    x = pre * _sigmoid(pre)
    x_dt = x * _pair(cols[:, 0:1], cols[:, 1:2])
    x_b = x_dt.astype(BF16)
    y_parts = []
    for c in range(2):
        lo, hi = c * CHUNK, (c + 1) * CHUNK
        heads = [_dot((g_sc[c] * _decay(rows, cols, c, h)).astype(BF16), x_b[lo:hi]) for h in range(2)]
        y_parts.append(_pair(heads[0], heads[1]))
    state, _, _ = _state(x_dt, rows, cols, b_sc)
    from_start = jnp.exp(_pair(cols[CHUNK:, 2:3], cols[CHUNK:, 3:4]))
    y_parts[1] += from_start * _dot_dims(c_sc[pl.ds(CHUNK, CHUNK), :], state, NT)
    lane0 = pl.multiple_of(j * LANES, LANES)
    y = jnp.concatenate(y_parts, axis=0) + par_ref[1:2, pl.ds(lane0, LANES)] * x
    y_ref[ALL] = y
    z = z_ref[ALL].astype(F32)
    v = y * (z * _sigmoid(z))
    v_sc[j] = v
    acc[ALL] += v * v

    @pl.when(j == N_PAIRS - 1)
    def _():
        r = lax.rsqrt(_sum(acc[ALL], 1) / D_INNER + NORM_EPS)
        r_full = jnp.broadcast_to(r, (SEQ, LANES))
        r_ref[ALL] = r_full

        @pl.loop(0, N_PAIRS)
        def _(i):
            at = pl.ds(pl.multiple_of(i * LANES, LANES), LANES)
            n_ref[:, at] = (v_sc[i] * r_full * par_ref[0:1, at]).astype(BF16)


def bwd_kernel(rows_ref, x_ref, z_ref, b_ref, c_ref, y_ref, dn_ref, r_ref, tx_ref, tb_ref, tc_ref, par_ref,
               dp_ref, drows_ref, gch_ref, gbc_ref, b_sc, c_sc, g_sc, dg_sc, dc_sc, db_sc, acc, pad, pad_out):
    phase, j = pl.program_id(0), pl.program_id(1)
    gate = par_ref[0:1]
    skip = par_ref[1:2]
    z = z_ref[ALL].astype(F32)
    sig_z = _sigmoid(z)
    act_z = z * sig_z
    y = y_ref[ALL]
    v = y * act_z
    d_n = dn_ref[ALL].astype(F32)
    d_vn = d_n * gate

    @pl.when(phase == 0)
    def _():
        @pl.when(j == 0)
        def _():
            acc[ALL] = jnp.zeros_like(acc)

        acc[ALL] += d_vn * v

    @pl.when(phase == 1)
    def _():
        @pl.when(j == 0)
        def _():
            total = _sum(acc[ALL], 1) / D_INNER
            acc[ALL] = jnp.broadcast_to(total, (SEQ, LANES))
            _scores(b_ref, c_ref, tb_ref, tc_ref, b_sc, c_sc, g_sc, pad)
            dg_sc[ALL] = jnp.zeros_like(dg_sc)
            dc_sc[ALL] = jnp.zeros_like(dc_sc)
            db_sc[ALL] = jnp.zeros_like(db_sc)

        r = r_ref[ALL]
        d_v = r * d_vn - v * (r * r * r) * acc[ALL]
        g_gate = _sum(d_n * v * r, 0)
        lane0 = pl.multiple_of(j * LANES, LANES)
        dp_ref[:, pl.ds(lane0, LANES)] = (d_v * y * _silu_grad(z, sig_z)).astype(BF16)
        d_y = d_v * act_z

        rows = rows_ref[0]
        cols = rows.T
        _fill(pad, x_ref[ALL].astype(F32))
        pre = _conv(pad, tx_ref[ALL])
        sig_x = _sigmoid(pre)
        x = pre * sig_x
        dt = _pair(cols[:, 0:1], cols[:, 1:2])
        x_dt = x * dt
        x_b = x_dt.astype(BF16)
        x_r = x_b.astype(F32)
        g_skip = _sum(d_y * x, 0)
        dy_b = d_y.astype(BF16)
        dy_r = dy_b.astype(F32)
        dy_t = dy_r.T.astype(BF16)
        first = _iota((CHUNK, LANES), 1) < HEAD
        dx_parts = []
        for c in range(2):
            lo, hi = c * CHUNK, (c + 1) * CHUNK
            halves = []
            for h in range(2):
                decay = _decay(rows, cols, c, h)
                mixed = (g_sc[c] * decay).astype(BF16)
                own = first if h == 0 else jnp.logical_not(first)
                dy_h = jnp.where(own, dy_r[lo:hi], 0.0).astype(BF16)
                dg_sc[c] += _dot_dims(dy_h, x_b[lo:hi], NT) * decay
                halves.append(_dot(dy_t[h * HEAD:(h + 1) * HEAD, lo:hi], mixed))
            dx_parts.append(jnp.concatenate(halves, axis=0).T)
        state, x_end, weight = _state(x_dt, rows, cols, b_sc)
        dy_off = dy_r[CHUNK:] * jnp.exp(_pair(cols[CHUNK:, 2:3], cols[CHUNK:, 3:4]))
        dc_sc[ALL] += _dot(dy_off.astype(BF16), state)
        d_state = _dot(dy_off.T.astype(BF16), c_sc[pl.ds(CHUNK, CHUNK), :]).astype(BF16)
        db_sc[ALL] += _dot(x_end, d_state)
        dx_state = weight * _dot_dims(b_sc[pl.ds(0, CHUNK), :], d_state, NT)
        dx_parts[0] += dx_state
        d_xdt = jnp.concatenate(dx_parts, axis=0)
        end_sum = _sum(x_r[:CHUNK] * dx_state, 0)
        d_cum = dy_r * (y - skip * x) - x_r * d_xdt
        d_cum += jnp.where(_iota((SEQ, LANES), 0) == CHUNK - 1, end_sum, 0.0)
        dt_t = (d_xdt * x).T
        cum_t = d_cum.T
        drows_ref[0] = jnp.concatenate(
            [_sum(part[h * HEAD:(h + 1) * HEAD], 0) for part in (dt_t, cum_t) for h in range(2)]
            + [jnp.zeros((4, SEQ), F32)], axis=0)
        d_pre = (d_xdt * dt + skip * d_y) * _silu_grad(pre, sig_x)
        d_in, g_rows = _conv_back(pad_out, d_pre, pad, tx_ref[ALL])
        dp_ref[:, pl.ds(pl.multiple_of(D_INNER + lane0, LANES), LANES)] = d_in.astype(BF16)
        gch_ref[ALL] = jnp.concatenate(g_rows + [g_gate, g_skip, jnp.zeros((1, LANES), F32)], axis=0)

        @pl.when(j == N_PAIRS - 1)
        def _():
            causal = _iota((CHUNK, CHUNK), 0) >= _iota((CHUNK, CHUNK), 1)
            d_b, d_c = [], []
            for c in range(2):
                sl = pl.ds(c * CHUNK, CHUNK)
                d_g = jnp.where(causal, dg_sc[c], 0.0)
                d_c.append(_dot(d_g.astype(BF16), b_sc[sl, :]))
                d_b.append(_dot(d_g.T.astype(BF16), c_sc[sl, :]))
            d_c[1] += dc_sc[ALL]
            d_b[0] += db_sc[ALL]
            for i, (parts, ref, taps) in enumerate(((d_b, b_ref, tb_ref), (d_c, c_ref, tc_ref))):
                _fill(pad, ref[ALL].astype(F32))
                pre_i = _conv(pad, taps[ALL])
                d_pre_i = jnp.concatenate(parts, axis=0) * _silu_grad(pre_i, _sigmoid(pre_i))
                d_val, g_val = _conv_back(pad_out, d_pre_i, pad, taps[ALL])
                dp_ref[:, pl.ds(2 * D_INNER + i * LANES, LANES)] = d_val.astype(BF16)
                gbc_ref[:, pl.ds(i * LANES, LANES)] = jnp.concatenate(g_val + [jnp.zeros((3, LANES), F32)], axis=0)
            dp_ref[:, pl.ds(2 * D_INNER + 2 * LANES, LANES)] = jnp.zeros((SEQ, LANES), BF16)


def _col(block):
    return pl.BlockSpec((SEQ, LANES), lambda j: (0, block(j)))


def mixer_fwd(proj, rows, taps, par):
    taps_at = lambda block: pl.BlockSpec((8, LANES), lambda j: (0, block(j)))
    return pl.pallas_call(
        fwd_kernel,
        grid=(N_PAIRS,),
        in_specs=[
            pl.BlockSpec((1, 8, SEQ), lambda j: (j, 0, 0)),
            _col(lambda j: N_PAIRS + j), _col(lambda j: j), _col(lambda j: 2 * N_PAIRS), _col(lambda j: 2 * N_PAIRS + 1),
            taps_at(lambda j: j), taps_at(lambda j: N_PAIRS), taps_at(lambda j: N_PAIRS + 1),
            pl.BlockSpec((8, D_INNER), lambda j: (0, 0)),
        ],
        out_specs=[_col(lambda j: j), pl.BlockSpec((SEQ, D_INNER), lambda j: (0, 0)), pl.BlockSpec((SEQ, LANES), lambda j: (0, 0))],
        out_shape=[
            jax.ShapeDtypeStruct((SEQ, D_INNER), F32),
            jax.ShapeDtypeStruct((SEQ, D_INNER), BF16),
            jax.ShapeDtypeStruct((SEQ, LANES), F32),
        ],
        scratch_shapes=[
            pltpu.VMEM((SEQ, LANES), BF16), pltpu.VMEM((SEQ, LANES), BF16), pltpu.VMEM((2, CHUNK, CHUNK), F32),
            pltpu.VMEM((N_PAIRS, SEQ, LANES), F32), pltpu.VMEM((SEQ, LANES), F32), pltpu.VMEM((SEQ + 2 * PAD, LANES), F32),
        ],
        compiler_params=pltpu.CompilerParams(dimension_semantics=("arbitrary",), vmem_limit_bytes=40 * 2 ** 20),
        cost_estimate=pl.CostEstimate(flops=8 * 10 ** 9, bytes_accessed=16 * 10 ** 6, transcendentals=10 ** 7),
        name="mixer_fwd",
    )(rows, proj, proj, proj, proj, taps, taps, taps, par)


def mixer_bwd(proj, rows, taps, par, y, d_n, r):
    col = lambda block: pl.BlockSpec((SEQ, LANES), lambda f, j: (0, block(f, j)))
    taps_at = lambda block: pl.BlockSpec((8, LANES), lambda f, j: (0, block(f, j)))
    return pl.pallas_call(
        bwd_kernel,
        grid=(2, N_PAIRS),
        in_specs=[
            pl.BlockSpec((1, 8, SEQ), lambda f, j: (f * j, 0, 0)),
            col(lambda f, j: N_PAIRS + f * j), col(lambda f, j: j), col(lambda f, j: 2 * N_PAIRS), col(lambda f, j: 2 * N_PAIRS + 1),
            col(lambda f, j: j), col(lambda f, j: j), col(lambda f, j: 0),
            taps_at(lambda f, j: f * j), taps_at(lambda f, j: N_PAIRS), taps_at(lambda f, j: N_PAIRS + 1), taps_at(lambda f, j: j),
        ],
        out_specs=[
            pl.BlockSpec((SEQ, PROJ_PAD), lambda f, j: (0, 0)),
            pl.BlockSpec((1, 8, SEQ), lambda f, j: (f * j, 0, 0)),
            taps_at(lambda f, j: f * j),
            pl.BlockSpec((8, 2 * LANES), lambda f, j: (0, 0)),
        ],
        out_shape=[
            jax.ShapeDtypeStruct((SEQ, PROJ_PAD), BF16),
            jax.ShapeDtypeStruct((N_PAIRS, 8, SEQ), F32),
            jax.ShapeDtypeStruct((8, D_INNER), F32),
            jax.ShapeDtypeStruct((8, 2 * LANES), F32),
        ],
        scratch_shapes=[
            pltpu.VMEM((SEQ, LANES), BF16), pltpu.VMEM((SEQ, LANES), BF16), pltpu.VMEM((2, CHUNK, CHUNK), F32),
            pltpu.VMEM((2, CHUNK, CHUNK), F32), pltpu.VMEM((CHUNK, LANES), F32), pltpu.VMEM((CHUNK, LANES), F32),
            pltpu.VMEM((SEQ, LANES), F32), pltpu.VMEM((SEQ + 2 * PAD, LANES), F32), pltpu.VMEM((SEQ + 2 * PAD, LANES), F32),
        ],
        compiler_params=pltpu.CompilerParams(dimension_semantics=("arbitrary", "arbitrary"), vmem_limit_bytes=40 * 2 ** 20),
        cost_estimate=pl.CostEstimate(flops=16 * 10 ** 9, bytes_accessed=40 * 10 ** 6, transcendentals=10 ** 7),
        name="mixer_bwd",
    )(rows, proj, proj, proj, proj, y, d_n, r, taps, taps, taps, par)


IN_PART = 800
OUT_PART = 192
UNITS = ((0, 0, IN_PART), (0, 4 * IN_PART, IN_PART), (1, 0, OUT_PART))
N_UNITS = 2 * len(UNITS)


def gather_kernel(win_ref, wout_ref, in_a, out_a, in_b, out_b, buf_in, buf_out, sends, recvs, tails, tailr, loads, stores):
    i, d = lax.axis_index('fsdp'), lax.axis_index('dp')
    x, c, z, y = i // 2, i % 2, d // 2, d % 2
    chip_x, core = 2 * (1 - x) + c, 2 * x + (1 - c)
    near_y, near_z = 2 * z + (1 - y), 2 * (1 - z) + y
    to_x, to_core = {'dp': d, 'fsdp': chip_x}, {'dp': d, 'fsdp': core}
    to_y, to_z = {'dp': near_y, 'fsdp': i}, {'dp': near_z, 'fsdp': i}

    barrier = pltpu.get_barrier_semaphore()
    for device in (to_x, to_core, to_y, to_z):
        pl.semaphore_signal(barrier, inc=1, device_id=device, device_id_type=pl.DeviceIdType.MESH)
    pl.semaphore_wait(barrier, 4)

    fulls = ((in_a, out_a), (in_b, out_b))
    pieces, bufs = (win_ref, wout_ref), (buf_in, buf_out)

    def source(u, row, size):
        layer, (kind, _, _) = u // 3, UNITS[u % 3]
        return pieces[kind].at[layer, pl.ds(row, size), :]

    def place(u, piece, row, size):
        layer, (kind, _, _) = u // 3, UNITS[u % 3]
        if kind == 0:
            return fulls[layer][0].at[pl.ds(row, size), pl.ds(pl.multiple_of(piece * 384, 128), 384)]
        return fulls[layer][1].at[pl.ds(pl.multiple_of(piece * 768 + row, 16), size), :]

    def span(u, q):
        _, first, size = UNITS[u % 3]
        return pl.multiple_of(first + q * size, 16), size

    def copy(u, slot, src, dst, device):
        return pltpu.make_async_remote_copy(
            src_ref=src, dst_ref=dst, send_sem=sends.at[u, slot], recv_sem=recvs.at[u, slot],
            device_id=device, device_id_type=pl.DeviceIdType.MESH)

    def forward(u, slot, piece, row, size, device):
        return copy(u, slot, place(u, piece, row, size), place(u, piece, row, size), device)

    started = []

    def go(op):
        op.start()
        started.append(op)

    def tail_copy(layer, slot, src, device):
        dst = fulls[layer][0].at[pl.ds(8 * IN_PART, N_HEADS), pl.ds(pl.multiple_of((i if slot < 2 else chip_x) * 384, 128), 384)]
        return pltpu.make_async_remote_copy(
            src_ref=src, dst_ref=dst, send_sem=tails.at[layer, slot], recv_sem=tailr.at[layer, slot],
            device_id=device, device_id_type=pl.DeviceIdType.MESH)

    for u in range(N_UNITS):
        row, size = span(u, d)
        go(copy(u, 0, source(u, row, size), place(u, i, row, size), to_x))
    tails_own = []
    for layer in range(2):
        src = win_ref.at[layer, pl.ds(8 * IN_PART, N_HEADS), :]
        for slot, device in ((0, to_x), (1, to_core)):
            op = tail_copy(layer, slot, src, device)
            op.start()
            tails_own.append(op)
    for u in range(N_UNITS):
        _, first, size = UNITS[u % 3]
        go(copy(u, 5, source(u, first, 4 * size), place(u, i, first, 4 * size), to_core))

    local_in = [pltpu.make_async_copy(pieces[kind].at[layer], bufs[kind].at[layer], loads.at[layer, kind])
                for layer in range(2) for kind in range(2)]
    for op in local_in:
        op.start()
    local_out = []
    for n, op in enumerate(local_in):
        layer, kind = n // 2, n % 2
        op.wait()
        if kind == 0:
            dst = fulls[layer][0].at[:, pl.ds(pl.multiple_of(i * 384, 128), 384)]
        else:
            dst = fulls[layer][1].at[pl.ds(pl.multiple_of(i * 768, 16), 768), :]
        out = pltpu.make_async_copy(bufs[kind].at[layer], dst, stores.at[layer, kind])
        out.start()
        local_out.append(out)

    def got(u, slot, piece, row, size):
        forward(u, slot, piece, row, size, to_core).wait_recv()

    def stage_one(u):
        row, size = span(u, d)
        got(u, 0, chip_x, row, size)
        go(forward(u, 1, chip_x, row, size, to_y))
        go(forward(u, 2, chip_x, row, size, to_z))
        go(forward(u, 6, chip_x, row, size, to_core))

    def stage_two(u):
        half = UNITS[u % 3][2] // 2
        row, size = span(u, near_y)
        got(u, 1, chip_x, row, size)
        go(forward(u, 3, chip_x, row, half, to_z))
        go(forward(u, 7, chip_x, row, size, to_core))
        row, size = span(u, near_z)
        got(u, 2, chip_x, row, size)
        go(forward(u, 4, chip_x, row + half, half, to_y))
        go(forward(u, 8, chip_x, row, size, to_core))

    def stage_three(u):
        half = UNITS[u % 3][2] // 2
        row, _ = span(u, 2 * (1 - z) + (1 - y))
        got(u, 3, chip_x, row, half)
        go(forward(u, 9, chip_x, row, half, to_core))
        got(u, 4, chip_x, row + half, half)
        go(forward(u, 10, chip_x, row + half, half, to_core))

    for t in range(N_UNITS + 2):
        if t < N_UNITS:
            stage_one(t)
        if 0 <= t - 1 < N_UNITS:
            stage_two(t - 1)
        if 0 <= t - 2:
            stage_three(t - 2)

    for layer in range(2):
        tail_at = fulls[layer][0].at[pl.ds(8 * IN_PART, N_HEADS), pl.ds(pl.multiple_of(chip_x * 384, 128), 384)]
        tail_copy(layer, 0, win_ref.at[layer, pl.ds(8 * IN_PART, N_HEADS), :], to_x).wait_recv()
        op = tail_copy(layer, 2, tail_at, to_core)
        op.start()
        tails_own.append(op)

    diag, other_core_x = 2 * (1 - z) + (1 - y), 2 * (1 - x) + (1 - c)
    for u in range(N_UNITS):
        _, first, size = UNITS[u % 3]
        half = size // 2
        got(u, 5, core, first, 4 * size)
        for slot, q in ((6, d), (7, near_y), (8, near_z)):
            row, _ = span(u, q)
            got(u, slot, other_core_x, row, size)
        row, _ = span(u, diag)
        got(u, 9, other_core_x, row, half)
        got(u, 10, other_core_x, row + half, half)
    for layer in range(2):
        for slot in (1, 2):
            tail_copy(layer, slot, win_ref.at[layer, pl.ds(8 * IN_PART, N_HEADS), :], to_core).wait_recv()
    for op in started + tails_own:
        op.wait_send()
    for op in local_out:
        op.wait()


def gather_weights(w_in_t, w_out):
    full = [jax.ShapeDtypeStruct((PROJ, D_MODEL), BF16), jax.ShapeDtypeStruct((D_INNER, D_MODEL), BF16)]
    hbm = pl.BlockSpec(memory_space=pltpu.HBM)
    return pl.pallas_call(
        gather_kernel,
        in_specs=[hbm, hbm],
        out_specs=[hbm] * 4,
        out_shape=full + full,
        scratch_shapes=[
            pltpu.VMEM(w_in_t.shape, BF16), pltpu.VMEM(w_out.shape, BF16),
            pltpu.SemaphoreType.DMA((N_UNITS, 11)), pltpu.SemaphoreType.DMA((N_UNITS, 11)),
            pltpu.SemaphoreType.DMA((2, 3)), pltpu.SemaphoreType.DMA((2, 3)),
            pltpu.SemaphoreType.DMA((2, 2)), pltpu.SemaphoreType.DMA((2, 2)),
        ],
        compiler_params=pltpu.CompilerParams(collective_id=0, has_side_effects=True, vmem_limit_bytes=40 * 2 ** 20),
        cost_estimate=pl.CostEstimate(flops=10 ** 9, bytes_accessed=10 ** 8, transcendentals=0),
        name="gather_weights",
    )(w_in_t, w_out)


def pre_norm(u_rows, norm_w):
    rows_f = u_rows.astype(F32)
    inv_rms = lax.rsqrt(jnp.mean(jnp.square(rows_f), axis=-1, keepdims=True) + NORM_EPS)
    return (rows_f * inv_rms * norm_w.astype(F32)).astype(BF16)


def head_rows(dt_raw, dt_bias, a_log):
    dt = jax.nn.softplus(dt_raw.astype(F32) + dt_bias).T
    a = dt * -jnp.exp(a_log)[:, None]
    upto = (jnp.arange(CHUNK)[:, None] <= jnp.arange(CHUNK)[None, :]).astype(F32)
    cum = jnp.einsum('hcs,st->hct', a.reshape(N_HEADS, SEQ // CHUNK, CHUNK), upto, precision=lax.Precision.HIGHEST)
    pairs = (N_PAIRS, 2, SEQ)
    return jnp.concatenate([dt.reshape(pairs), cum.reshape(pairs), jnp.zeros((N_PAIRS, 4, SEQ), F32)], axis=1)


def layer_forward(u_rows, small, w_in, w_out):
    norm_w, taps, par, dt_bias, a_log = small
    h_norm, norm_pull = jax.vjp(pre_norm, u_rows, norm_w)
    proj = lax.dot_general(h_norm, w_in, NT, preferred_element_type=F32).astype(BF16)
    rows, rows_pull = jax.vjp(head_rows, proj[:, 2 * D_INNER + 2 * LANES:], dt_bias, a_log)
    y, y_norm, r = mixer_fwd(proj, rows, taps, par)
    out = (u_rows.astype(F32) + jnp.dot(y_norm, w_out, preferred_element_type=F32)).astype(BF16)
    return out, (h_norm, norm_pull, proj, rows, rows_pull, y, y_norm, r)


COL_CHUNKS = ((0, 2176), (2176, 4352), (4352, 6528))


def solution(mesh):
    dp_size = mesh.shape['dp']
    fsdp_size = mesh.shape['fsdp']
    act_spec = P(('dp', 'fsdp'), None, None)
    weight_specs = (P(None, 'fsdp'), P(None, 'fsdp', None), P(None, None, 'fsdp'), P(None, 'fsdp'), P(None, 'fsdp'), P(None, 'fsdp'), P(None, 'fsdp'), P(None, 'fsdp'), P(None, 'fsdp', None))

    def per_device(u_loc, g_loc, norm_w, w_in, conv_w, conv_b, dt_bias, a_log, d_skip, gate_w, w_out):
        batch_tot = dp_size * fsdp_size
        me_dp = lax.axis_index('dp')
        me_fsdp = lax.axis_index('fsdp')

        small_pieces = [norm_w, conv_w.reshape(2, -1), conv_b, gate_w, dt_bias, a_log, d_skip]
        widths = [piece.shape[1] for piece in small_pieces]
        packed = jnp.concatenate([piece.astype(F32) for piece in small_pieces], axis=1)
        gathered = lax.all_gather(packed, 'fsdp', axis=0)
        w_in, w_out, gathered = lax.optimization_barrier((w_in, w_out, gathered))

        def small_layer(layer):
            vals, at = [], 0
            for width in widths:
                vals.append(gathered[:, layer, at:at + width])
                at += width
            norm, cw, cb, gate, bias, alog, skip = vals
            taps = jnp.concatenate([
                cw.reshape(fsdp_size, 4, -1).transpose(1, 0, 2).reshape(4, CONV_DIM), cb.reshape(1, CONV_DIM),
                jnp.zeros((3, CONV_DIM), F32)], axis=0)
            par = jnp.concatenate([
                gate.reshape(1, D_INNER), jnp.repeat(skip.reshape(N_HEADS), HEAD).reshape(1, D_INNER),
                jnp.zeros((6, D_INNER), F32)], axis=0)
            return norm.reshape(D_MODEL), taps, par, bias.reshape(N_HEADS), alog.reshape(N_HEADS)

        chip, core = me_fsdp // 2, me_fsdp % 2
        swap = lambda k: [(i, i ^ k) for i in range(4)]

        def by_core(left):
            size = left.shape[1] // 4
            return [jnp.concatenate([lax.dynamic_slice_in_dim(left, (2 * half + at) * size, size, 1) for half in range(2)], axis=1)
                    for at in (1 - core, core)]

        def partial_grad(left, right):
            return (lax.dot_general(left, right, TN, preferred_element_type=F32) / batch_tot).astype(BF16)

        def spread(sent, kept, axis):
            got = lax.ppermute(sent, 'fsdp', swap(1))
            chip_u, got = lax.optimization_barrier((chip, got))
            pair = kept + got
            size = pair.shape[axis] // 2
            got = lax.ppermute(lax.dynamic_slice_in_dim(pair, (1 - chip_u) * size, size, axis), 'fsdp', swap(2))
            dp_u, got = lax.optimization_barrier((me_dp, got))
            piece = lax.dynamic_slice_in_dim(pair, chip_u * size, size, axis) + got
            quarters = piece.reshape(dp_size, piece.shape[0] // dp_size, piece.shape[1])
            terms = [lax.dynamic_index_in_dim(quarters, dp_u ^ k, 0, keepdims=False) for k in range(dp_size)]
            for k in range(1, dp_size):
                terms[k] = lax.ppermute(terms[k], 'dp', swap(k))
            terms = [term.astype(F32) for term in terms]
            total = (terms[0] + terms[1]) + (terms[2] + terms[3])
            return lax.all_gather(total, 'dp', axis=0, tiled=True)

        def layer_backward(d_out, saved, small, full_in, full_out):
            _, taps, par, _, _ = small
            h_norm, norm_pull, proj, rows, rows_pull, y, y_norm, r = saved
            y_other, y_own = by_core(y_norm)
            sent = partial_grad(y_other, d_out)
            d_out, sent = lax.optimization_barrier((d_out, sent))
            out_parts = spread(sent, partial_grad(y_own, d_out), 0)
            d_n = lax.dot_general(d_out, full_out, NT, preferred_element_type=F32).astype(BF16)
            d_proj, d_rows, g_ch, g_bc = mixer_bwd(proj, rows, taps, par, y, d_n, r)
            d_raw, g_bias, g_alog = rows_pull(d_rows)
            d_proj = lax.dynamic_update_slice(d_proj, d_raw, (0, 2 * D_INNER + 2 * LANES))
            h_other, h_own = by_core(h_norm)
            cols = [d_proj[:, lo:hi] for lo, hi in COL_CHUNKS]
            sent, kept = [], []
            for col in cols:
                sent.append(partial_grad(col, h_other))
            for col in cols:
                kept.append(partial_grad(col, h_own))
            d_proj, _, _ = lax.optimization_barrier((d_proj, sent, kept))
            in_parts = [spread(a, b, 1) for a, b in zip(sent, kept)]
            d_h = jnp.dot(d_proj[:, :PROJ], full_in, preferred_element_type=F32).astype(BF16)
            d_u_norm, g_norm = norm_pull(d_h)
            d_u = (d_out.astype(F32) + d_u_norm.astype(F32)).astype(BF16)
            g_conv = jnp.concatenate([g_ch[:5], g_bc[:5]], axis=1)
            g_skip = jnp.sum(g_ch[6].reshape(N_HEADS, HEAD), axis=1)
            smalls = [g_norm, g_conv[:4], g_conv[4], g_ch[5], g_bias, g_alog, g_skip]
            return d_u, out_parts, in_parts, smalls

        u_rows, d_out = u_loc[0], g_loc[0]
        small_one, small_two = small_layer(0), small_layer(1)
        in_one, out_one, in_two, out_two = gather_weights(w_in.swapaxes(1, 2), w_out)
        hidden, saved_one = layer_forward(u_rows, small_one, in_one, out_one)
        out_rows, saved_two = layer_forward(hidden, small_two, in_two, out_two)
        d_hidden, out_parts_two, in_parts_two, smalls_two = layer_backward(d_out, saved_two, small_two, in_two, out_two)
        d_u, out_parts_one, in_parts_one, smalls_one = layer_backward(d_hidden, saved_one, small_one, in_one, out_one)

        g_in = jnp.zeros((2, PROJ, w_in.shape[1]), F32)
        g_out = jnp.zeros((2,) + w_out.shape[1:], F32)
        for layer, in_parts, out_part in ((1, in_parts_two, out_parts_two), (0, in_parts_one, out_parts_one)):
            g_out = lax.dynamic_update_slice(g_out, out_part[None], (layer, 0, 0))
            for (lo, hi), part in zip(COL_CHUNKS, in_parts):
                g_in = lax.dynamic_update_slice(g_in, part[None, :min(hi, PROJ) - lo], (layer, lo, 0))

        def small_piece_rows(smalls):
            vals = []
            for idx, grad in enumerate(smalls):
                grad = grad.astype(F32) / batch_tot
                if idx < 4:
                    grad = grad.astype(BF16).astype(F32)
                if idx == 1:
                    grad = grad.reshape(4, fsdp_size, -1).transpose(1, 0, 2)
                vals.append(grad.reshape(fsdp_size, -1))
            return jnp.concatenate(vals, axis=1)

        both = jnp.stack([small_piece_rows(smalls_one), small_piece_rows(smalls_two)], axis=1)
        for axis in ('fsdp', 'dp'):
            for k in (1, 2):
                both = both + lax.ppermute(both, axis, swap(k))
        summed = lax.dynamic_index_in_dim(both, me_fsdp, 0, keepdims=False)
        outs, at = [], 0
        for width in widths:
            outs.append(summed[:, at:at + width])
            at += width
        g_norm, g_cw, g_cb, g_gate, g_bias, g_alog, g_skip = outs
        return (out_rows[None], d_u[None], g_norm, g_in.swapaxes(1, 2), g_cw.reshape(conv_w.shape), g_cb, g_bias, g_alog, g_skip, g_gate, g_out)

    return jax.shard_map(per_device, mesh=mesh, in_specs=(act_spec, act_spec) + weight_specs, out_specs=(act_spec, act_spec) + weight_specs, check_vma=False)
```

```python
import jax
import jax.numpy as jnp
from jax import lax
from jax.experimental import pallas as pl
from jax.experimental.pallas import tpu as pltpu
from jax.sharding import PartitionSpec as P


ALL = Ellipsis
CHUNK = 256
SEQ = 512
LANES = 128
PAD = 8
HEAD = 64
D_MODEL = 1536
D_INNER = 3072
N_HEADS = 48
CONV_DIM = 3328
PROJ = 6448
PROJ_PAD = 6528
N_PAIRS = N_HEADS // 2
NORM_EPS = 1e-5
F32 = jnp.float32
BF16 = jnp.bfloat16
NT = (((1,), (1,)), ((), ()))
TN = (((0,), (0,)), ((), ()))


def _dot(a, b):
    return jnp.dot(a, b, preferred_element_type=F32)


def _dot_dims(a, b, dims):
    return lax.dot_general(a, b, dims, preferred_element_type=F32)


def _sum(x, axis):
    return jnp.sum(x, axis=axis, keepdims=True)


def _iota(shape, dim):
    return lax.broadcasted_iota(jnp.int32, shape, dim)


def _fill(pad, x):
    zeros = jnp.zeros((PAD, LANES), F32)
    pad[pl.ds(0, PAD), :] = zeros
    pad[pl.ds(PAD, SEQ), :] = x
    pad[pl.ds(PAD + SEQ, PAD), :] = zeros


def _shift(pad, k):
    return pad[pl.ds(PAD + k, SEQ), :]


def _conv(pad, taps):
    out = taps[4:5] + _shift(pad, 0) * taps[3:4]
    for k in range(3):
        out += _shift(pad, k - 3) * taps[k:k + 1]
    return out


def _conv_back(pad_out, d_out, pad_in, taps):
    _fill(pad_out, d_out)
    d_in = d_out * taps[3:4]
    for k in range(3):
        d_in += _shift(pad_out, 3 - k) * taps[k:k + 1]
    rows = [_sum(d_out * _shift(pad_in, k - 3), 0) for k in range(4)]
    rows.append(_sum(d_out, 0))
    return d_in, rows


def _sigmoid(x):
    return 0.5 * jnp.tanh(0.5 * x) + 0.5


def _silu_grad(x, sig):
    return sig * (1.0 + x * (1.0 - sig))


def _pair(a, b):
    shape = (max(a.shape[0], b.shape[0]), LANES)
    return jnp.where(_iota(shape, 1) < HEAD, a, b)


def _scores(b_ref, c_ref, tb_ref, tc_ref, b_sc, c_sc, g_sc, pad):
    for ref, taps, dst in ((b_ref, tb_ref, b_sc), (c_ref, tc_ref, c_sc)):
        _fill(pad, ref[ALL].astype(F32))
        pre = _conv(pad, taps[ALL])
        dst[ALL] = (pre * _sigmoid(pre)).astype(BF16)
    causal = _iota((CHUNK, CHUNK), 0) >= _iota((CHUNK, CHUNK), 1)
    for c in range(2):
        sl = pl.ds(c * CHUNK, CHUNK)
        g_sc[c] = jnp.where(causal, _dot_dims(c_sc[sl, :], b_sc[sl, :], NT), 0.0)


def _decay(rows, cols, c, h):
    lo, hi = c * CHUNK, (c + 1) * CHUNK
    return jnp.exp(jnp.minimum(cols[lo:hi, 2 + h:3 + h] - rows[2 + h:3 + h, lo:hi], 0.0))


def _state(x_dt, rows, cols, b_sc):
    end = _pair(rows[2:3, CHUNK - 1:CHUNK], rows[3:4, CHUNK - 1:CHUNK])
    weight = jnp.exp(jnp.minimum(end - _pair(cols[:CHUNK, 2:3], cols[:CHUNK, 3:4]), 0.0))
    x_end = (x_dt[:CHUNK] * weight).astype(BF16)
    state = _dot_dims(x_end, b_sc[pl.ds(0, CHUNK), :], TN).astype(BF16)
    return state, x_end, weight


def fwd_kernel(rows_ref, x_ref, z_ref, b_ref, c_ref, tx_ref, tb_ref, tc_ref, par_ref,
               y_ref, n_ref, r_ref, b_sc, c_sc, g_sc, v_sc, acc, pad):
    j = pl.program_id(0)

    @pl.when(j == 0)
    def _():
        _scores(b_ref, c_ref, tb_ref, tc_ref, b_sc, c_sc, g_sc, pad)
        acc[ALL] = jnp.zeros_like(acc)

    rows = rows_ref[0]
    cols = rows.T
    _fill(pad, x_ref[ALL].astype(F32))
    pre = _conv(pad, tx_ref[ALL])
    x = pre * _sigmoid(pre)
    x_dt = x * _pair(cols[:, 0:1], cols[:, 1:2])
    x_b = x_dt.astype(BF16)
    y_parts = []
    for c in range(2):
        lo, hi = c * CHUNK, (c + 1) * CHUNK
        heads = [_dot((g_sc[c] * _decay(rows, cols, c, h)).astype(BF16), x_b[lo:hi]) for h in range(2)]
        y_parts.append(_pair(heads[0], heads[1]))
    state, _, _ = _state(x_dt, rows, cols, b_sc)
    from_start = jnp.exp(_pair(cols[CHUNK:, 2:3], cols[CHUNK:, 3:4]))
    y_parts[1] += from_start * _dot_dims(c_sc[pl.ds(CHUNK, CHUNK), :], state, NT)
    lane0 = pl.multiple_of(j * LANES, LANES)
    y = jnp.concatenate(y_parts, axis=0) + par_ref[1:2, pl.ds(lane0, LANES)] * x
    y_ref[ALL] = y
    z = z_ref[ALL].astype(F32)
    v = y * (z * _sigmoid(z))
    v_sc[j] = v
    acc[ALL] += v * v

    @pl.when(j == N_PAIRS - 1)
    def _():
        r = lax.rsqrt(_sum(acc[ALL], 1) / D_INNER + NORM_EPS)
        r_full = jnp.broadcast_to(r, (SEQ, LANES))
        r_ref[ALL] = r_full

        @pl.loop(0, N_PAIRS)
        def _(i):
            at = pl.ds(pl.multiple_of(i * LANES, LANES), LANES)
            n_ref[:, at] = (v_sc[i] * r_full * par_ref[0:1, at]).astype(BF16)


def bwd_kernel(rows_ref, x_ref, z_ref, b_ref, c_ref, y_ref, dn_ref, r_ref, tx_ref, tb_ref, tc_ref, par_ref,
               dp_ref, drows_ref, gch_ref, gbc_ref, b_sc, c_sc, g_sc, dg_sc, dc_sc, db_sc, acc, pad, pad_out):
    phase, j = pl.program_id(0), pl.program_id(1)
    gate = par_ref[0:1]
    skip = par_ref[1:2]
    z = z_ref[ALL].astype(F32)
    sig_z = _sigmoid(z)
    act_z = z * sig_z
    y = y_ref[ALL]
    v = y * act_z
    d_n = dn_ref[ALL].astype(F32)
    d_vn = d_n * gate

    @pl.when(phase == 0)
    def _():
        @pl.when(j == 0)
        def _():
            acc[ALL] = jnp.zeros_like(acc)

        acc[ALL] += d_vn * v

    @pl.when(phase == 1)
    def _():
        @pl.when(j == 0)
        def _():
            total = _sum(acc[ALL], 1) / D_INNER
            acc[ALL] = jnp.broadcast_to(total, (SEQ, LANES))
            _scores(b_ref, c_ref, tb_ref, tc_ref, b_sc, c_sc, g_sc, pad)
            dg_sc[ALL] = jnp.zeros_like(dg_sc)
            dc_sc[ALL] = jnp.zeros_like(dc_sc)
            db_sc[ALL] = jnp.zeros_like(db_sc)

        r = r_ref[ALL]
        d_v = r * d_vn - v * (r * r * r) * acc[ALL]
        g_gate = _sum(d_n * v * r, 0)
        lane0 = pl.multiple_of(j * LANES, LANES)
        dp_ref[:, pl.ds(lane0, LANES)] = (d_v * y * _silu_grad(z, sig_z)).astype(BF16)
        d_y = d_v * act_z

        rows = rows_ref[0]
        cols = rows.T
        _fill(pad, x_ref[ALL].astype(F32))
        pre = _conv(pad, tx_ref[ALL])
        sig_x = _sigmoid(pre)
        x = pre * sig_x
        dt = _pair(cols[:, 0:1], cols[:, 1:2])
        x_dt = x * dt
        x_b = x_dt.astype(BF16)
        x_r = x_b.astype(F32)
        g_skip = _sum(d_y * x, 0)
        dy_b = d_y.astype(BF16)
        dy_r = dy_b.astype(F32)
        dy_t = dy_r.T.astype(BF16)
        first = _iota((CHUNK, LANES), 1) < HEAD
        dx_parts = []
        for c in range(2):
            lo, hi = c * CHUNK, (c + 1) * CHUNK
            halves = []
            for h in range(2):
                decay = _decay(rows, cols, c, h)
                mixed = (g_sc[c] * decay).astype(BF16)
                own = first if h == 0 else jnp.logical_not(first)
                dy_h = jnp.where(own, dy_r[lo:hi], 0.0).astype(BF16)
                dg_sc[c] += _dot_dims(dy_h, x_b[lo:hi], NT) * decay
                halves.append(_dot(dy_t[h * HEAD:(h + 1) * HEAD, lo:hi], mixed))
            dx_parts.append(jnp.concatenate(halves, axis=0).T)
        state, x_end, weight = _state(x_dt, rows, cols, b_sc)
        dy_off = dy_r[CHUNK:] * jnp.exp(_pair(cols[CHUNK:, 2:3], cols[CHUNK:, 3:4]))
        dc_sc[ALL] += _dot(dy_off.astype(BF16), state)
        d_state = _dot(dy_off.T.astype(BF16), c_sc[pl.ds(CHUNK, CHUNK), :]).astype(BF16)
        db_sc[ALL] += _dot(x_end, d_state)
        dx_state = weight * _dot_dims(b_sc[pl.ds(0, CHUNK), :], d_state, NT)
        dx_parts[0] += dx_state
        d_xdt = jnp.concatenate(dx_parts, axis=0)
        end_sum = _sum(x_r[:CHUNK] * dx_state, 0)
        d_cum = dy_r * (y - skip * x) - x_r * d_xdt
        d_cum += jnp.where(_iota((SEQ, LANES), 0) == CHUNK - 1, end_sum, 0.0)
        dt_t = (d_xdt * x).T
        cum_t = d_cum.T
        drows_ref[0] = jnp.concatenate(
            [_sum(part[h * HEAD:(h + 1) * HEAD], 0) for part in (dt_t, cum_t) for h in range(2)]
            + [jnp.zeros((4, SEQ), F32)], axis=0)
        d_pre = (d_xdt * dt + skip * d_y) * _silu_grad(pre, sig_x)
        d_in, g_rows = _conv_back(pad_out, d_pre, pad, tx_ref[ALL])
        dp_ref[:, pl.ds(pl.multiple_of(D_INNER + lane0, LANES), LANES)] = d_in.astype(BF16)
        gch_ref[ALL] = jnp.concatenate(g_rows + [g_gate, g_skip, jnp.zeros((1, LANES), F32)], axis=0)

        @pl.when(j == N_PAIRS - 1)
        def _():
            causal = _iota((CHUNK, CHUNK), 0) >= _iota((CHUNK, CHUNK), 1)
            d_b, d_c = [], []
            for c in range(2):
                sl = pl.ds(c * CHUNK, CHUNK)
                d_g = jnp.where(causal, dg_sc[c], 0.0)
                d_c.append(_dot(d_g.astype(BF16), b_sc[sl, :]))
                d_b.append(_dot(d_g.T.astype(BF16), c_sc[sl, :]))
            d_c[1] += dc_sc[ALL]
            d_b[0] += db_sc[ALL]
            for i, (parts, ref, taps) in enumerate(((d_b, b_ref, tb_ref), (d_c, c_ref, tc_ref))):
                _fill(pad, ref[ALL].astype(F32))
                pre_i = _conv(pad, taps[ALL])
                d_pre_i = jnp.concatenate(parts, axis=0) * _silu_grad(pre_i, _sigmoid(pre_i))
                d_val, g_val = _conv_back(pad_out, d_pre_i, pad, taps[ALL])
                dp_ref[:, pl.ds(2 * D_INNER + i * LANES, LANES)] = d_val.astype(BF16)
                gbc_ref[:, pl.ds(i * LANES, LANES)] = jnp.concatenate(g_val + [jnp.zeros((3, LANES), F32)], axis=0)
            dp_ref[:, pl.ds(2 * D_INNER + 2 * LANES, LANES)] = jnp.zeros((SEQ, LANES), BF16)


def _col(block):
    return pl.BlockSpec((SEQ, LANES), lambda j: (0, block(j)))


def mixer_fwd(proj, rows, taps, par):
    taps_at = lambda block: pl.BlockSpec((8, LANES), lambda j: (0, block(j)))
    return pl.pallas_call(
        fwd_kernel,
        grid=(N_PAIRS,),
        in_specs=[
            pl.BlockSpec((1, 8, SEQ), lambda j: (j, 0, 0)),
            _col(lambda j: N_PAIRS + j), _col(lambda j: j), _col(lambda j: 2 * N_PAIRS), _col(lambda j: 2 * N_PAIRS + 1),
            taps_at(lambda j: j), taps_at(lambda j: N_PAIRS), taps_at(lambda j: N_PAIRS + 1),
            pl.BlockSpec((8, D_INNER), lambda j: (0, 0)),
        ],
        out_specs=[_col(lambda j: j), pl.BlockSpec((SEQ, D_INNER), lambda j: (0, 0)), pl.BlockSpec((SEQ, LANES), lambda j: (0, 0))],
        out_shape=[
            jax.ShapeDtypeStruct((SEQ, D_INNER), F32),
            jax.ShapeDtypeStruct((SEQ, D_INNER), BF16),
            jax.ShapeDtypeStruct((SEQ, LANES), F32),
        ],
        scratch_shapes=[
            pltpu.VMEM((SEQ, LANES), BF16), pltpu.VMEM((SEQ, LANES), BF16), pltpu.VMEM((2, CHUNK, CHUNK), F32),
            pltpu.VMEM((N_PAIRS, SEQ, LANES), F32), pltpu.VMEM((SEQ, LANES), F32), pltpu.VMEM((SEQ + 2 * PAD, LANES), F32),
        ],
        compiler_params=pltpu.CompilerParams(dimension_semantics=("arbitrary",), vmem_limit_bytes=40 * 2 ** 20),
        cost_estimate=pl.CostEstimate(flops=8 * 10 ** 9, bytes_accessed=16 * 10 ** 6, transcendentals=10 ** 7),
        name="mixer_fwd",
    )(rows, proj, proj, proj, proj, taps, taps, taps, par)


def mixer_bwd(proj, rows, taps, par, y, d_n, r):
    col = lambda block: pl.BlockSpec((SEQ, LANES), lambda f, j: (0, block(f, j)))
    taps_at = lambda block: pl.BlockSpec((8, LANES), lambda f, j: (0, block(f, j)))
    return pl.pallas_call(
        bwd_kernel,
        grid=(2, N_PAIRS),
        in_specs=[
            pl.BlockSpec((1, 8, SEQ), lambda f, j: (f * j, 0, 0)),
            col(lambda f, j: N_PAIRS + f * j), col(lambda f, j: j), col(lambda f, j: 2 * N_PAIRS), col(lambda f, j: 2 * N_PAIRS + 1),
            col(lambda f, j: j), col(lambda f, j: j), col(lambda f, j: 0),
            taps_at(lambda f, j: f * j), taps_at(lambda f, j: N_PAIRS), taps_at(lambda f, j: N_PAIRS + 1), taps_at(lambda f, j: j),
        ],
        out_specs=[
            pl.BlockSpec((SEQ, PROJ_PAD), lambda f, j: (0, 0)),
            pl.BlockSpec((1, 8, SEQ), lambda f, j: (f * j, 0, 0)),
            taps_at(lambda f, j: f * j),
            pl.BlockSpec((8, 2 * LANES), lambda f, j: (0, 0)),
        ],
        out_shape=[
            jax.ShapeDtypeStruct((SEQ, PROJ_PAD), BF16),
            jax.ShapeDtypeStruct((N_PAIRS, 8, SEQ), F32),
            jax.ShapeDtypeStruct((8, D_INNER), F32),
            jax.ShapeDtypeStruct((8, 2 * LANES), F32),
        ],
        scratch_shapes=[
            pltpu.VMEM((SEQ, LANES), BF16), pltpu.VMEM((SEQ, LANES), BF16), pltpu.VMEM((2, CHUNK, CHUNK), F32),
            pltpu.VMEM((2, CHUNK, CHUNK), F32), pltpu.VMEM((CHUNK, LANES), F32), pltpu.VMEM((CHUNK, LANES), F32),
            pltpu.VMEM((SEQ, LANES), F32), pltpu.VMEM((SEQ + 2 * PAD, LANES), F32), pltpu.VMEM((SEQ + 2 * PAD, LANES), F32),
        ],
        compiler_params=pltpu.CompilerParams(dimension_semantics=("arbitrary", "arbitrary"), vmem_limit_bytes=40 * 2 ** 20),
        cost_estimate=pl.CostEstimate(flops=16 * 10 ** 9, bytes_accessed=40 * 10 ** 6, transcendentals=10 ** 7),
        name="mixer_bwd",
    )(rows, proj, proj, proj, proj, y, d_n, r, taps, taps, taps, par)


IN_PART = 800
UNITS = ((0, IN_PART), (4 * IN_PART, IN_PART))
N_UNITS = 2 * len(UNITS)


def gather_kernel(win_ref, in_a, in_b, buf_in, sends, recvs, tails, tailr, loads, stores):
    i, d = lax.axis_index('fsdp'), lax.axis_index('dp')
    x, c, z, y = i // 2, i % 2, d // 2, d % 2
    chip_x, core = 2 * (1 - x) + c, 2 * x + (1 - c)
    near_y, near_z = 2 * z + (1 - y), 2 * (1 - z) + y
    to_x, to_core = {'dp': d, 'fsdp': chip_x}, {'dp': d, 'fsdp': core}
    to_y, to_z = {'dp': near_y, 'fsdp': i}, {'dp': near_z, 'fsdp': i}

    barrier = pltpu.get_barrier_semaphore()
    for device in (to_x, to_core, to_y, to_z):
        pl.semaphore_signal(barrier, inc=1, device_id=device, device_id_type=pl.DeviceIdType.MESH)
    pl.semaphore_wait(barrier, 4)

    fulls = (in_a, in_b)
    units = len(UNITS)

    def source(u, row, size):
        return win_ref.at[u // units, pl.ds(row, size), :]

    def place(u, piece, row, size):
        return fulls[u // units].at[pl.ds(row, size), pl.ds(pl.multiple_of(piece * 384, 128), 384)]

    def span(u, q):
        first, size = UNITS[u % units]
        return pl.multiple_of(first + q * size, 16), size

    def copy(u, slot, src, dst, device):
        return pltpu.make_async_remote_copy(
            src_ref=src, dst_ref=dst, send_sem=sends.at[u, slot], recv_sem=recvs.at[u, slot],
            device_id=device, device_id_type=pl.DeviceIdType.MESH)

    def forward(u, slot, piece, row, size, device):
        return copy(u, slot, place(u, piece, row, size), place(u, piece, row, size), device)

    started = []

    def go(op):
        op.start()
        started.append(op)

    def tail_copy(layer, slot, src, device):
        dst = fulls[layer].at[pl.ds(8 * IN_PART, N_HEADS), pl.ds(pl.multiple_of((i if slot < 2 else chip_x) * 384, 128), 384)]
        return pltpu.make_async_remote_copy(
            src_ref=src, dst_ref=dst, send_sem=tails.at[layer, slot], recv_sem=tailr.at[layer, slot],
            device_id=device, device_id_type=pl.DeviceIdType.MESH)

    for u in range(N_UNITS):
        row, size = span(u, d)
        go(copy(u, 0, source(u, row, size), place(u, i, row, size), to_x))
    tails_own = []
    for layer in range(2):
        src = win_ref.at[layer, pl.ds(8 * IN_PART, N_HEADS), :]
        for slot, device in ((0, to_x), (1, to_core)):
            op = tail_copy(layer, slot, src, device)
            op.start()
            tails_own.append(op)
    for u in range(N_UNITS):
        first, size = UNITS[u % units]
        go(copy(u, 5, source(u, first, 4 * size), place(u, i, first, 4 * size), to_core))

    local_in = [pltpu.make_async_copy(win_ref.at[layer], buf_in.at[layer], loads.at[layer]) for layer in range(2)]
    for op in local_in:
        op.start()
    local_out = []
    for layer, op in enumerate(local_in):
        op.wait()
        dst = fulls[layer].at[:, pl.ds(pl.multiple_of(i * 384, 128), 384)]
        out = pltpu.make_async_copy(buf_in.at[layer], dst, stores.at[layer])
        out.start()
        local_out.append(out)

    def got(u, slot, piece, row, size):
        forward(u, slot, piece, row, size, to_core).wait_recv()

    def stage_one(u):
        row, size = span(u, d)
        got(u, 0, chip_x, row, size)
        go(forward(u, 1, chip_x, row, size, to_y))
        go(forward(u, 2, chip_x, row, size, to_z))
        go(forward(u, 6, chip_x, row, size, to_core))

    def stage_two(u):
        half = UNITS[u % units][1] // 2
        row, size = span(u, near_y)
        got(u, 1, chip_x, row, size)
        go(forward(u, 3, chip_x, row, half, to_z))
        go(forward(u, 7, chip_x, row, size, to_core))
        row, size = span(u, near_z)
        got(u, 2, chip_x, row, size)
        go(forward(u, 4, chip_x, row + half, half, to_y))
        go(forward(u, 8, chip_x, row, size, to_core))

    def stage_three(u):
        half = UNITS[u % units][1] // 2
        row, _ = span(u, 2 * (1 - z) + (1 - y))
        got(u, 3, chip_x, row, half)
        go(forward(u, 9, chip_x, row, half, to_core))
        got(u, 4, chip_x, row + half, half)
        go(forward(u, 10, chip_x, row + half, half, to_core))

    for t in range(N_UNITS + 2):
        if t < N_UNITS:
            stage_one(t)
        if 0 <= t - 1 < N_UNITS:
            stage_two(t - 1)
        if 0 <= t - 2:
            stage_three(t - 2)

    for layer in range(2):
        tail_at = fulls[layer].at[pl.ds(8 * IN_PART, N_HEADS), pl.ds(pl.multiple_of(chip_x * 384, 128), 384)]
        tail_copy(layer, 0, win_ref.at[layer, pl.ds(8 * IN_PART, N_HEADS), :], to_x).wait_recv()
        op = tail_copy(layer, 2, tail_at, to_core)
        op.start()
        tails_own.append(op)

    diag, other_core_x = 2 * (1 - z) + (1 - y), 2 * (1 - x) + (1 - c)
    for u in range(N_UNITS):
        first, size = UNITS[u % units]
        half = size // 2
        got(u, 5, core, first, 4 * size)
        for slot, q in ((6, d), (7, near_y), (8, near_z)):
            row, _ = span(u, q)
            got(u, slot, other_core_x, row, size)
        row, _ = span(u, diag)
        got(u, 9, other_core_x, row, half)
        got(u, 10, other_core_x, row + half, half)
    for layer in range(2):
        for slot in (1, 2):
            tail_copy(layer, slot, win_ref.at[layer, pl.ds(8 * IN_PART, N_HEADS), :], to_core).wait_recv()
    for op in started + tails_own:
        op.wait_send()
    for op in local_out:
        op.wait()


def gather_w_in(w_in_t):
    hbm = pl.BlockSpec(memory_space=pltpu.HBM)
    return pl.pallas_call(
        gather_kernel,
        in_specs=[hbm],
        out_specs=[hbm] * 2,
        out_shape=[jax.ShapeDtypeStruct((PROJ, D_MODEL), BF16)] * 2,
        scratch_shapes=[
            pltpu.VMEM(w_in_t.shape, BF16),
            pltpu.SemaphoreType.DMA((N_UNITS, 11)), pltpu.SemaphoreType.DMA((N_UNITS, 11)),
            pltpu.SemaphoreType.DMA((2, 3)), pltpu.SemaphoreType.DMA((2, 3)),
            pltpu.SemaphoreType.DMA((2,)), pltpu.SemaphoreType.DMA((2,)),
        ],
        compiler_params=pltpu.CompilerParams(collective_id=0, has_side_effects=True, vmem_limit_bytes=40 * 2 ** 20),
        cost_estimate=pl.CostEstimate(flops=10 ** 9, bytes_accessed=10 ** 8, transcendentals=0),
        name="gather_w_in",
    )(w_in_t)


def pre_norm(u_rows, norm_w):
    rows_f = u_rows.astype(F32)
    inv_rms = lax.rsqrt(jnp.mean(jnp.square(rows_f), axis=-1, keepdims=True) + NORM_EPS)
    return (rows_f * inv_rms * norm_w.astype(F32)).astype(BF16)


def head_rows(dt_raw, dt_bias, a_log):
    dt = jax.nn.softplus(dt_raw.astype(F32) + dt_bias).T
    a = dt * -jnp.exp(a_log)[:, None]
    upto = (jnp.arange(CHUNK)[:, None] <= jnp.arange(CHUNK)[None, :]).astype(F32)
    cum = jnp.einsum('hcs,st->hct', a.reshape(N_HEADS, SEQ // CHUNK, CHUNK), upto, precision=lax.Precision.HIGHEST)
    pairs = (N_PAIRS, 2, SEQ)
    return jnp.concatenate([dt.reshape(pairs), cum.reshape(pairs), jnp.zeros((N_PAIRS, 4, SEQ), F32)], axis=1)


def layer_forward(u_rows, small, w_in, w_out):
    norm_w, taps, par, dt_bias, a_log = small
    h_norm, norm_pull = jax.vjp(pre_norm, u_rows, norm_w)
    proj = lax.dot_general(h_norm, w_in, NT, preferred_element_type=F32).astype(BF16)
    rows, rows_pull = jax.vjp(head_rows, proj[:, 2 * D_INNER + 2 * LANES:], dt_bias, a_log)
    y, y_norm, r = mixer_fwd(proj, rows, taps, par)
    out = (u_rows.astype(F32) + jnp.dot(y_norm, w_out, preferred_element_type=F32)).astype(BF16)
    return out, (h_norm, norm_pull, proj, rows, rows_pull, y, y_norm, r)


COL_CHUNKS = ((0, 2176), (2176, 4352), (4352, 6528))


def solution(mesh):
    dp_size = mesh.shape['dp']
    fsdp_size = mesh.shape['fsdp']
    act_spec = P(('dp', 'fsdp'), None, None)
    weight_specs = (P(None, 'fsdp'), P(None, 'fsdp', None), P(None, None, 'fsdp'), P(None, 'fsdp'), P(None, 'fsdp'), P(None, 'fsdp'), P(None, 'fsdp'), P(None, 'fsdp'), P(None, 'fsdp', None))

    def per_device(u_loc, g_loc, norm_w, w_in, conv_w, conv_b, dt_bias, a_log, d_skip, gate_w, w_out):
        batch_tot = dp_size * fsdp_size
        me_dp = lax.axis_index('dp')
        me_fsdp = lax.axis_index('fsdp')

        small_pieces = [norm_w, conv_w.reshape(2, -1), conv_b, gate_w, dt_bias, a_log, d_skip]
        widths = [piece.shape[1] for piece in small_pieces]
        packed = jnp.concatenate([piece.astype(F32) for piece in small_pieces], axis=1)
        gathered = lax.all_gather(packed, 'fsdp', axis=0)
        w_in, gathered = lax.optimization_barrier((w_in, gathered))

        def small_layer(layer):
            vals, at = [], 0
            for width in widths:
                vals.append(gathered[:, layer, at:at + width])
                at += width
            norm, cw, cb, gate, bias, alog, skip = vals
            taps = jnp.concatenate([
                cw.reshape(fsdp_size, 4, -1).transpose(1, 0, 2).reshape(4, CONV_DIM), cb.reshape(1, CONV_DIM),
                jnp.zeros((3, CONV_DIM), F32)], axis=0)
            par = jnp.concatenate([
                gate.reshape(1, D_INNER), jnp.repeat(skip.reshape(N_HEADS), HEAD).reshape(1, D_INNER),
                jnp.zeros((6, D_INNER), F32)], axis=0)
            return norm.reshape(D_MODEL), taps, par, bias.reshape(N_HEADS), alog.reshape(N_HEADS)

        chip, core = me_fsdp // 2, me_fsdp % 2
        swap = lambda k: [(i, i ^ k) for i in range(4)]

        def by_core(left):
            size = left.shape[1] // 4
            return [jnp.concatenate([lax.dynamic_slice_in_dim(left, (2 * half + at) * size, size, 1) for half in range(2)], axis=1)
                    for at in (1 - core, core)]

        def partial_grad(left, right):
            return (lax.dot_general(left, right, TN, preferred_element_type=F32) / batch_tot).astype(BF16)

        def spread(sent, kept, axis):
            got = lax.ppermute(sent, 'fsdp', swap(1))
            chip_u, got = lax.optimization_barrier((chip, got))
            pair = kept + got
            size = pair.shape[axis] // 2
            got = lax.ppermute(lax.dynamic_slice_in_dim(pair, (1 - chip_u) * size, size, axis), 'fsdp', swap(2))
            dp_u, got = lax.optimization_barrier((me_dp, got))
            piece = lax.dynamic_slice_in_dim(pair, chip_u * size, size, axis) + got
            quarters = piece.reshape(dp_size, piece.shape[0] // dp_size, piece.shape[1])
            terms = [lax.dynamic_index_in_dim(quarters, dp_u ^ k, 0, keepdims=False) for k in range(dp_size)]
            for k in range(1, dp_size):
                terms[k] = lax.ppermute(terms[k], 'dp', swap(k))
            terms = [term.astype(F32) for term in terms]
            total = (terms[0] + terms[1]) + (terms[2] + terms[3])
            return lax.all_gather(total, 'dp', axis=0, tiled=True)

        def layer_backward(d_out, saved, small, full_in, full_out):
            _, taps, par, _, _ = small
            h_norm, norm_pull, proj, rows, rows_pull, y, y_norm, r = saved
            y_other, y_own = by_core(y_norm)
            sent = partial_grad(y_other, d_out)
            d_out, sent = lax.optimization_barrier((d_out, sent))
            out_parts = spread(sent, partial_grad(y_own, d_out), 0)
            d_n = lax.dot_general(d_out, full_out, NT, preferred_element_type=F32).astype(BF16)
            d_proj, d_rows, g_ch, g_bc = mixer_bwd(proj, rows, taps, par, y, d_n, r)
            d_raw, g_bias, g_alog = rows_pull(d_rows)
            d_proj = lax.dynamic_update_slice(d_proj, d_raw, (0, 2 * D_INNER + 2 * LANES))
            h_other, h_own = by_core(h_norm)
            cols = [d_proj[:, lo:hi] for lo, hi in COL_CHUNKS]
            sent, kept = [], []
            for col in cols:
                sent.append(partial_grad(col, h_other))
            for col in cols:
                kept.append(partial_grad(col, h_own))
            d_proj, _, _ = lax.optimization_barrier((d_proj, sent, kept))
            in_parts = [spread(a, b, 1) for a, b in zip(sent, kept)]
            d_h = jnp.dot(d_proj[:, :PROJ], full_in, preferred_element_type=F32).astype(BF16)
            d_u_norm, g_norm = norm_pull(d_h)
            d_u = (d_out.astype(F32) + d_u_norm.astype(F32)).astype(BF16)
            g_conv = jnp.concatenate([g_ch[:5], g_bc[:5]], axis=1)
            g_skip = jnp.sum(g_ch[6].reshape(N_HEADS, HEAD), axis=1)
            smalls = [g_norm, g_conv[:4], g_conv[4], g_ch[5], g_bias, g_alog, g_skip]
            return d_u, out_parts, in_parts, smalls

        u_rows, d_out = u_loc[0], g_loc[0]
        small_one, small_two = small_layer(0), small_layer(1)
        out_one = lax.all_gather(w_out[0], 'fsdp', axis=0, tiled=True)
        out_two = lax.all_gather(w_out[1], 'fsdp', axis=0, tiled=True)
        in_one, in_two = gather_w_in(w_in.swapaxes(1, 2))
        hidden, saved_one = layer_forward(u_rows, small_one, in_one, out_one)
        out_rows, saved_two = layer_forward(hidden, small_two, in_two, out_two)
        d_hidden, out_parts_two, in_parts_two, smalls_two = layer_backward(d_out, saved_two, small_two, in_two, out_two)
        d_u, out_parts_one, in_parts_one, smalls_one = layer_backward(d_hidden, saved_one, small_one, in_one, out_one)

        g_in = jnp.zeros((2, PROJ, w_in.shape[1]), F32)
        g_out = jnp.zeros((2,) + w_out.shape[1:], F32)
        for layer, in_parts, out_part in ((1, in_parts_two, out_parts_two), (0, in_parts_one, out_parts_one)):
            g_out = lax.dynamic_update_slice(g_out, out_part[None], (layer, 0, 0))
            for (lo, hi), part in zip(COL_CHUNKS, in_parts):
                g_in = lax.dynamic_update_slice(g_in, part[None, :min(hi, PROJ) - lo], (layer, lo, 0))

        def small_piece_rows(smalls):
            vals = []
            for idx, grad in enumerate(smalls):
                grad = grad.astype(F32) / batch_tot
                if idx < 4:
                    grad = grad.astype(BF16).astype(F32)
                if idx == 1:
                    grad = grad.reshape(4, fsdp_size, -1).transpose(1, 0, 2)
                vals.append(grad.reshape(fsdp_size, -1))
            return jnp.concatenate(vals, axis=1)

        both = jnp.stack([small_piece_rows(smalls_one), small_piece_rows(smalls_two)], axis=1)
        for axis in ('fsdp', 'dp'):
            for k in (1, 2):
                both = both + lax.ppermute(both, axis, swap(k))
        summed = lax.dynamic_index_in_dim(both, me_fsdp, 0, keepdims=False)
        outs, at = [], 0
        for width in widths:
            outs.append(summed[:, at:at + width])
            at += width
        g_norm, g_cw, g_cb, g_gate, g_bias, g_alog, g_skip = outs
        return (out_rows[None], d_u[None], g_norm, g_in.swapaxes(1, 2), g_cw.reshape(conv_w.shape), g_cb, g_bias, g_alog, g_skip, g_gate, g_out)

    return jax.shard_map(per_device, mesh=mesh, in_specs=(act_spec, act_spec) + weight_specs, out_specs=(act_spec, act_spec) + weight_specs, check_vma=False)
```
